32 devices in a mesh: dp: 4 (over y, z), tp: 8 (over x, core).
Axes of the slice: x: 4, y: 2, z: 2, core: 2. Of those that a mesh axis runs over, the one named last changes fastest.
The devices are a block of a 4x4x8 slice.
Arguments:
- hidden: bfloat16 [4096, 1152], P('dp'), parts along dimension 0
- norm_gain: float32 [1152], replicated
- emb_table: bfloat16 [16384, 1152], P('tp')
- teacher_ids: int32 [4096, 256], P('dp'), parts along dimension 0
- teacher_q: float32 [4096, 256], P('dp'), parts along dimension 0
Outputs:
- output 1: float32 [4], P('dp'), parts along dimension 0
- output 2: bfloat16 [4096, 1152], P('dp'), parts along dimension 0
- output 3: float32 [4608], P('dp'), parts along dimension 0
- output 4: float32 [65536, 1152], P(('dp', 'tp')), parts along dimension 0
There are 4 independent parts. The reference program is written for one: setup_inputs(seed, part) draws one part's arguments, and reference() takes and returns one part's arrays. A program takes and returns all parts, laid end to end along the dimension named above; an argument that names none is the same for every part.
All inputs are finite; a program needn't handle non-finite values.
Results may differ from the reference program's by a relative error of at most 0.00161376.
Values sent between devices are 32-bit elements.
A program may use at most 768 MiB of HBM per device.

```python
import math
import jax
import jax.numpy as jnp
from jax import lax

TOKENS = 1024
VOCAB = 16384
D = 1152
TEACHER_K = 256


def norm_apply(hid_f, gain_vec):
    inv_rms = lax.rsqrt(jnp.mean(hid_f * hid_f, axis=-1, keepdims=True) + 1e-6)
    return hid_f * inv_rms * (1.0 + gain_vec)


def draw_ids(key_ids):
    hot_count = TEACHER_K - TEACHER_K // 2
    cold_count = TEACHER_K // 2
    stride = (VOCAB - 2 * hot_count) // cold_count
    key_bit, key_jit, key_perm = jax.random.split(key_ids, 3)
    hot_ids = 2 * jnp.arange(hot_count)[None, :] + jax.random.randint(key_bit, (TOKENS, hot_count), 0, 2)
    cold_ids = 2 * hot_count + stride * jnp.arange(cold_count)[None, :] + jax.random.randint(key_jit, (TOKENS, cold_count), 0, stride)
    hot_ids = hot_ids.at[0].set(2 * jnp.arange(hot_count))
    cold_ids = cold_ids.at[0].set(2 * hot_count + stride * jnp.arange(cold_count) + stride - 1)
    all_ids = jnp.concatenate([hot_ids, cold_ids], axis=1)
    column_order = jax.random.permutation(key_perm, TEACHER_K)
    return all_ids[:, column_order].astype(jnp.int32)


def setup_inputs(seed: int = 0, part: int = 0) -> dict:
    root_key = jax.random.key(seed)
    key_tab, key_gain, key_dir = jax.random.split(root_key, 3)
    part_key = jax.random.fold_in(jax.random.key(seed + 1), part)
    key_hid, key_ids, key_wts = jax.random.split(part_key, 3)
    direction = jax.random.normal(key_dir, (D,), jnp.float32)
    direction = direction / jnp.sqrt(jnp.sum(direction * direction))
    spread = math.sqrt(0.5 * math.log(VOCAB) / D)
    offset = 24.0 / math.sqrt(D)
    emb_table = spread * jax.random.normal(key_tab, (VOCAB, D), jnp.float32) + offset * direction[None, :]
    norm_gain = 0.3 * jax.random.normal(key_gain, (D,), jnp.float32)
    hidden = jax.random.normal(key_hid, (TOKENS, D), jnp.float32) + 1.5 * math.sqrt(D) * direction[None, :]
    teacher_ids = draw_ids(key_ids)
    hot_mask = (teacher_ids < 2 * (TEACHER_K - TEACHER_K // 2)).astype(jnp.float32)
    scores = 0.8 * jax.random.normal(key_wts, (TOKENS, TEACHER_K), jnp.float32) + 0.5 * hot_mask
    teacher_q = jax.nn.softmax(scores, axis=-1)
    return {'hidden': hidden.astype(jnp.bfloat16), 'norm_gain': norm_gain, 'emb_table': emb_table.astype(jnp.bfloat16), 'teacher_ids': teacher_ids, 'teacher_q': teacher_q}


def reference(hidden, norm_gain, emb_table, teacher_ids, teacher_q):
    normed, norm_pull = jax.vjp(norm_apply, hidden.astype(jnp.float32), norm_gain)
    x_in = normed.astype(jnp.bfloat16)
    logits = jnp.dot(x_in, emb_table.T, preferred_element_type=jnp.float32)
    row_peak = jnp.max(logits, axis=1, keepdims=True)
    log_z = row_peak[:, 0] + jnp.log(jnp.sum(jnp.exp(logits - row_peak), axis=1))
    picked = jnp.take_along_axis(logits, teacher_ids, axis=1)
    q_total = jnp.sum(teacher_q, axis=1)
    token_loss = q_total * log_z - jnp.sum(teacher_q * picked, axis=1)
    mean_loss = jnp.mean(token_loss)[None]
    softmax_p = jnp.exp(logits - log_z[:, None])
    row_index = jnp.arange(TOKENS)[:, None]
    target_q = jnp.zeros((TOKENS, VOCAB), jnp.float32).at[row_index, teacher_ids].add(teacher_q)
    grad_z = ((softmax_p * q_total[:, None] - target_q) / TOKENS).astype(jnp.bfloat16)
    grad_x = jnp.dot(grad_z, emb_table, preferred_element_type=jnp.float32)
    grad_table = jnp.dot(grad_z.T, x_in, preferred_element_type=jnp.float32)
    grad_h, grad_gain = norm_pull(grad_x)
    return (mean_loss, grad_h.astype(jnp.bfloat16), grad_gain, grad_table)
```

```python
import functools

import jax
import jax.numpy as jnp
from jax import lax
from jax.experimental import pallas as pl
from jax.experimental.pallas import tpu as pltpu
from jax.sharding import PartitionSpec as P

LANES = 128
TILE = 256


def norm_apply(hid_f, gain_vec):
    inv_rms = lax.rsqrt(jnp.mean(hid_f * hid_f, axis=-1, keepdims=True) + 1e-6)
    return hid_f * inv_rms * (1.0 + gain_vec)


def build_targets(lo_ref, hi_ref, qh_ref, qm_ref, ql_ref, dense_ref, tokens, groups):
    count = lo_ref.shape[1]
    sub = 16
    base = lax.broadcasted_iota(jnp.int32, (sub, count), 0).astype(jnp.float32).astype(jnp.bfloat16)
    zero = jnp.zeros((sub, count), jnp.bfloat16)
    one = jnp.ones((sub, count), jnp.bfloat16)

    def row(ref, n):
        return jnp.broadcast_to(ref[pl.ds(n, 1), :], (sub, count)).astype(jnp.bfloat16)

    def one_token(n):
        lo, hi = row(lo_ref, n), row(hi_ref, n)
        low_hot = jnp.concatenate([jnp.where(lo == base + jnp.bfloat16(sub * k), one, zero) for k in range(LANES // sub)], axis=0)
        pieces = []
        for ref in (qh_ref, qm_ref, ql_ref):
            q = row(ref, n)
            for k in range(groups // sub):
                pieces.append(jnp.where(hi == base + jnp.bfloat16(sub * k), q, zero))
        lhs = jnp.concatenate(pieces, axis=0)
        out = lax.dot_general(lhs, low_hot, (((1,), (1,)), ((), ())), preferred_element_type=jnp.float32)
        total = out[:groups] + out[groups:2 * groups] + out[2 * groups:]
        dense_ref[pl.ds(n, groups, stride=tokens), :] = total

    unroll = 8

    @pl.loop(0, tokens // unroll)
    def _(i):
        for u in range(unroll):
            one_token(i * unroll + u)


def dz_kernel(scale, z_ref, lid_ref, q_ref, lz_ref, dz_ref, loss_ref, lo_s, hi_s, qh_s, qm_s, ql_s, dense_s):
    tokens, vocab = z_ref.shape
    groups = vocab // LANES
    lid = lid_ref[...]
    lo_s[...] = jnp.bitwise_and(lid, LANES - 1).astype(jnp.float32)
    hi_s[...] = jnp.right_shift(lid, 7).astype(jnp.float32)
    q = q_ref[...]
    qh = q.astype(jnp.bfloat16).astype(jnp.float32)
    rest = q - qh
    qm = rest.astype(jnp.bfloat16).astype(jnp.float32)
    qh_s[...] = qh
    qm_s[...] = qm
    ql_s[...] = rest - qm
    build_targets(lo_s, hi_s, qh_s, qm_s, ql_s, dense_s, tokens, groups)
    total = jnp.sum(q, axis=1, keepdims=True)
    part = jnp.zeros((8, LANES), jnp.float32)
    for r in range(0, tokens, LANES):
        rows = pl.ds(r, LANES)
        lz = lz_ref[rows, :]
        s = jnp.broadcast_to(total[r:r + LANES], (LANES, LANES))
        for g in range(groups):
            cols = pl.ds(g * LANES, LANES)
            z = z_ref[rows, cols]
            target = dense_s[pl.ds(g * tokens + r, LANES), :]
            dz_ref[rows, cols] = ((jnp.exp(z - lz) * s - target) * scale).astype(jnp.bfloat16)
            part += jnp.sum((target * z).reshape(LANES // 8, 8, LANES), axis=0)
    loss_ref[...] = part


def solution(mesh):
    def local_step(hidden, norm_gain, emb_block, teacher_ids, teacher_q):
        tokens = hidden.shape[0]
        vocab = emb_block.shape[0]
        count = teacher_ids.shape[1]
        block_start = lax.axis_index('tp') * vocab
        normed, norm_pull = jax.vjp(norm_apply, hidden.astype(jnp.float32), norm_gain)
        x_in = normed.astype(jnp.bfloat16)
        logits = lax.dot_general(x_in, emb_block, (((1,), (1,)), ((), ())), preferred_element_type=jnp.float32)
        row_peak = lax.pmax(jnp.max(logits, axis=1), 'tp')
        exp_total = lax.psum(jnp.sum(jnp.exp(logits - row_peak[:, None]), axis=1), 'tp')
        log_z = row_peak + jnp.log(exp_total)
        tile = min(TILE, tokens)
        steps = tokens // tile
        spec = lambda width: pl.BlockSpec((tile, width), lambda i: (i, 0))
        grad_z, loss_part = pl.pallas_call(
            functools.partial(dz_kernel, 1.0 / tokens),
            grid=(steps,),
            out_shape=(jax.ShapeDtypeStruct((tokens, vocab), jnp.bfloat16), jax.ShapeDtypeStruct((8 * steps, LANES), jnp.float32)),
            in_specs=[spec(vocab), spec(count), spec(count), spec(LANES)],
            out_specs=(spec(vocab), pl.BlockSpec((8, LANES), lambda i: (i, 0))),
            scratch_shapes=[pltpu.VMEM((tile, count), jnp.float32)] * 5 + [pltpu.VMEM((tile * vocab // LANES, LANES), jnp.float32)],
            compiler_params=pltpu.CompilerParams(vmem_limit_bytes=48 * 2**20),
            cost_estimate=pl.CostEstimate(flops=2 * 48 * 256 * 128 * tokens, bytes_accessed=12 * tokens * vocab // 2, transcendentals=tokens * vocab),
        )(logits, teacher_ids - block_start, teacher_q, jnp.broadcast_to(log_z[:, None], (tokens, LANES)))
        picked = lax.psum(jnp.sum(loss_part), 'tp')
        mean_loss = ((jnp.sum(jnp.sum(teacher_q, axis=1) * log_z) - picked) / tokens)[None]
        grad_part = jnp.dot(grad_z, emb_block, preferred_element_type=jnp.float32)
        grad_x = lax.psum(grad_part, 'tp')
        grad_block = lax.dot_general(grad_z, x_in, (((0,), (0,)), ((), ())), preferred_element_type=jnp.float32)
        grad_h, grad_gain = norm_pull(grad_x)
        return (mean_loss, grad_h.astype(jnp.bfloat16), grad_gain, grad_block)

    return jax.shard_map(local_step, mesh=mesh, in_specs=(P('dp', None), P(None), P('tp', None), P('dp', None), P('dp', None)), out_specs=(P('dp'), P('dp', None), P('dp'), P(('dp', 'tp'), None)), check_vma=False)
```

```python
import functools

import jax
import jax.numpy as jnp
from jax import lax
from jax.experimental import pallas as pl
from jax.experimental.pallas import tpu as pltpu
from jax.sharding import PartitionSpec as P

LANES = 128
CHUNK = 128
BLOCK = 256
UNROLL = 16
MESH = pl.DeviceIdType.MESH
LAG_A, LAG_B, LAG_C, LAG_D, LAG_E, LAG_F = 1, 2, 3, 4, 5, 6
(K_SIB, K_FAR_R, K_FAR_L, K_NEAR_R, K_NEAR_L, K_SUM_R, K_SUM_L, K_OUT_R, K_OUT_L, K_OUT_S,
 K_PASS_R, K_PASS_L, K_FWD_L, K_FWD_R, K_FWD_O) = range(15)
KINDS = 15


def build_targets(lo_ref, code_ref, pieces, dense_ref, tokens, groups):
    count = lo_ref.shape[1]
    sub, half = 16, LANES // 2
    base = lax.broadcasted_iota(jnp.int32, (sub, count), 0).astype(jnp.float32).astype(jnp.bfloat16)
    zero = jnp.zeros((sub, count), jnp.bfloat16)
    one = jnp.ones((sub, count), jnp.bfloat16)

    def row(ref, n):
        return jnp.broadcast_to(ref[pl.ds(n, 1), :], (sub, count)).astype(jnp.bfloat16)

    def one_token(n):
        lo, code = row(lo_ref, n), row(code_ref, n)
        weights = [row(ref, n) for ref in pieces]
        low_hot = jnp.concatenate([jnp.where(lo == base + jnp.bfloat16(sub * k), one, zero) for k in range(half // sub)], axis=0)
        here = [code == base + jnp.bfloat16(sub * k) for k in range(2 * groups // sub)]
        lhs = jnp.concatenate([jnp.where(h, w, zero) for w in weights for h in here], axis=0)
        out = lax.dot_general(lhs, low_hot, (((1,), (1,)), ((), ())), preferred_element_type=jnp.float32)
        out = out[:2 * groups] + out[2 * groups:4 * groups] + out[4 * groups:]
        dense_ref[pl.ds(n * (groups + 1), groups), :] = jnp.concatenate([out[:groups], out[groups:]], axis=1)

    @pl.loop(0, tokens // UNROLL)
    def _(i):
        for u in range(UNROLL):
            one_token(i * UNROLL + u)


def kernel(n_tp, hid_hbm, gain_ref, emb_hbm, ids_hbm, q_hbm, dh_hbm, x_hbm, dz_hbm, fin_ref,
           hid, emb, ids, q, xs, z, dz, lz_s, lo_s, code_s, qh_s, qm_s, ql_s, dense, part, sib_buf, ring_buf,
           grad, dh_s, dw_acc, loss_acc, slz_acc, stat_buf, fin_buf,
           in_sem, emb_sem, out_sem, dh_sem, x_sem, stat_send, stat_recv, fin_send, fin_recv, send_sem, recv_sem):
    tokens, width = hid.shape
    vocab = emb.shape[0]
    groups = vocab // LANES
    chunks = tokens // CHUNK
    chips = n_tp // 2
    half = CHUNK // 2
    own = half // chips
    bit = own // 2
    scale = 1.0 / tokens
    dp, me = lax.axis_index('dp'), lax.axis_index('tp')
    core = lax.rem(me, 2)
    chip = me // 2
    right = lax.rem(chip + 1, chips)
    left = lax.rem(chip + chips - 1, chips)
    far = lax.rem(chip + 2, chips)
    to_right, to_left, to_sib = right * 2 + core, left * 2 + core, chip * 2 + 1 - core

    barrier = pltpu.get_barrier_semaphore()
    for d in range(1, n_tp):
        pl.semaphore_signal(barrier, inc=1, device_id=(dp, lax.rem(me + d, n_tp)), device_id_type=MESH)

    get_hid = pltpu.make_async_copy(hid_hbm, hid, in_sem.at[0])
    get_ids = pltpu.make_async_copy(ids_hbm, ids, in_sem.at[1])
    get_q = pltpu.make_async_copy(q_hbm, q, in_sem.at[2])

    def get_emb(b):
        rows = pl.ds(pl.multiple_of(b * BLOCK, BLOCK), BLOCK)
        return pltpu.make_async_copy(emb_hbm.at[rows], emb.at[rows], emb_sem.at[b])

    get_hid.start()
    for b in range(vocab // BLOCK):
        get_emb(b).start()
    get_ids.start()
    get_q.start()

    get_hid.wait()
    gain = 1.0 + gain_ref[...]

    @pl.loop(0, tokens // 32)
    def _(i):
        rows = pl.ds(pl.multiple_of(i * 32, 32), 32)
        h = hid[rows, :].astype(jnp.float32)
        inv = lax.rsqrt(jnp.mean(h * h, axis=1, keepdims=True) + 1e-6)
        xs[rows, :] = (h * inv * gain).astype(jnp.bfloat16)

    put_x = pltpu.make_async_copy(xs, x_hbm, x_sem)
    put_x.start()

    @pl.loop(0, vocab // BLOCK)
    def _(b):
        get_emb(b).wait()
        rows = pl.ds(pl.multiple_of(b * BLOCK, BLOCK), BLOCK)
        for r in range(0, tokens, min(512, tokens)):
            z[b, pl.ds(r, min(512, tokens)), :] = lax.dot_general(xs[pl.ds(r, min(512, tokens)), :], emb[rows, :], (((1,), (1,)), ((), ())), preferred_element_type=jnp.float32)

    eye = lax.broadcasted_iota(jnp.int32, (LANES, LANES), 0) == lax.broadcasted_iota(jnp.int32, (LANES, LANES), 1)

    def as_row(tile):
        return jnp.sum(jnp.where(eye, tile, 0.0), axis=0, keepdims=True)

    stat_rows = tokens // LANES

    @pl.loop(0, stat_rows)
    def _(t):
        for u in range(0, LANES, 32):
            rows = pl.ds(pl.multiple_of(t * LANES + u, 32), 32)
            tiles = [z[g // 2, rows, pl.ds((g % 2) * LANES, LANES)] for g in range(groups)]
            peak = functools.reduce(jnp.maximum, tiles)
            peak = jnp.broadcast_to(jnp.max(peak, axis=1, keepdims=True), (32, LANES))
            total = functools.reduce(jnp.add, [jnp.exp(v - peak) for v in tiles])
            lz_s[rows, :] = peak
            dense[pl.ds(u, 32), :] = jnp.broadcast_to(jnp.sum(total, axis=1, keepdims=True), (32, LANES))
        stat_buf[me, pl.ds(t, 1), :] = as_row(lz_s[pl.ds(pl.multiple_of(t * LANES, LANES), LANES), :])
        stat_buf[me, pl.ds(stat_rows + t, 1), :] = as_row(dense[pl.ds(0, LANES), :])

    def everyone(buf, send, recv, d):
        return pltpu.make_async_remote_copy(
            src_ref=buf.at[me], dst_ref=buf.at[me], send_sem=send.at[d - 1], recv_sem=recv.at[d - 1],
            device_id=(dp, lax.rem(me + d, n_tp)), device_id_type=MESH)

    pl.semaphore_wait(barrier, n_tp - 1)
    for d in range(1, n_tp):
        everyone(stat_buf, stat_send, stat_recv, d).start()

    get_ids.wait()
    get_q.wait()
    start = me * vocab

    def prepare(c):
        @pl.loop(0, CHUNK // 32)
        def _(i):
            rows = pl.ds(pl.multiple_of(i * 32, 32), 32)
            src = pl.ds(pl.multiple_of(c * CHUNK + i * 32, 32), 32)
            lid = ids[src, :] - start
            lo_s[rows, :] = jnp.bitwise_and(lid, LANES // 2 - 1).astype(jnp.float32)
            code = jnp.right_shift(lid, 7) + groups * jnp.bitwise_and(jnp.right_shift(lid, 6), 1)
            code_s[rows, :] = jnp.where((lid >= 0) & (lid < vocab), code, -1).astype(jnp.float32)
            w = q[src, :] * scale
            wh = w.astype(jnp.bfloat16).astype(jnp.float32)
            rest = w - wh
            wm = rest.astype(jnp.bfloat16).astype(jnp.float32)
            qh_s[rows, :] = wh
            qm_s[rows, :] = wm
            ql_s[rows, :] = rest - wm

    prepare(0)
    build_targets(lo_s, code_s, (qh_s, qm_s, ql_s), dense, CHUNK, groups)

    for d in range(1, n_tp):
        everyone(stat_buf, stat_send, stat_recv, d).wait_recv()
    peaks = [stat_buf[k, pl.ds(0, stat_rows), :] for k in range(n_tp)]
    peak = functools.reduce(jnp.maximum, peaks)
    total = functools.reduce(jnp.add, [stat_buf[k, pl.ds(stat_rows, stat_rows), :] * jnp.exp(peaks[k] - peak) for k in range(n_tp)])
    log_z = peak + jnp.log(total)
    for t in range(stat_rows):
        tile = jnp.where(eye, jnp.broadcast_to(log_z[t:t + 1, :], (LANES, LANES)), 0.0)
        lz_s[pl.ds(t * LANES, LANES), :] = jnp.broadcast_to(jnp.sum(tile, axis=1, keepdims=True), (LANES, LANES))

    fin_buf[me] = jnp.zeros(fin_buf.shape[1:], jnp.float32)
    dw_acc[...] = jnp.zeros_like(dw_acc)
    loss_acc[...] = jnp.zeros_like(loss_acc)
    slz_acc[...] = jnp.zeros_like(slz_acc)

    mine = core * half
    theirs = half - mine

    def at(base, block, off=0):
        return base + block * own + off

    def rdma(c, kind):
        def rows(first, count):
            return pl.ds(pl.multiple_of(first, 8), count)

        if kind == K_SIB:
            src, dst, peer = part.at[c, rows(theirs, half)], sib_buf.at[c], to_sib
        elif kind in (K_FAR_R, K_FAR_L, K_NEAR_R, K_NEAR_L, K_SUM_R, K_SUM_L):
            first = {K_FAR_R: at(mine, far), K_FAR_L: at(mine, far, bit), K_NEAR_R: at(mine, right, bit),
                     K_NEAR_L: at(mine, left), K_SUM_R: at(mine, right), K_SUM_L: at(mine, left, bit)}[kind]
            src, dst = part.at[c, rows(first, bit)], ring_buf.at[c, kind - K_FAR_R]
            peer = to_right if kind in (K_FAR_R, K_NEAR_R, K_SUM_R) else to_left
        else:
            first, count, peer = {
                K_OUT_R: (at(mine, chip), own, to_right), K_OUT_L: (at(mine, chip), own, to_left), K_OUT_S: (at(mine, chip), own, to_sib),
                K_PASS_R: (at(mine, left), bit, to_right), K_PASS_L: (at(mine, right, bit), bit, to_left),
                K_FWD_L: (at(mine, left), own, to_sib), K_FWD_R: (at(mine, right), own, to_sib), K_FWD_O: (at(mine, far), own, to_sib)}[kind]
            src = dst = grad.at[c, rows(first, count)]
        return pltpu.make_async_remote_copy(src_ref=src, dst_ref=dst, send_sem=send_sem.at[c, kind], recv_sem=recv_sem.at[c, kind],
                                            device_id=(dp, peer), device_id_type=MESH)

    def put_dz(c):
        rows = pl.ds(pl.multiple_of(c * CHUNK, CHUNK), CHUNK)
        return pltpu.make_async_copy(dz.at[rows], dz_hbm.at[rows], out_sem.at[c])

    def put_dh(c):
        rows = pl.ds(pl.multiple_of(c * CHUNK, CHUNK), CHUNK)
        return pltpu.make_async_copy(dh_s.at[rows], dh_hbm.at[rows], dh_sem.at[c])

    def compute(c):
        sub = 32
        first = pl.multiple_of(c * CHUNK, CHUNK)

        @pl.loop(0, CHUNK // sub)
        def _(i):
            r = pl.multiple_of(i * sub, sub)
            rows = pl.ds(pl.multiple_of(first + r, sub), sub)
            lz = lz_s[rows, :]
            s = jnp.broadcast_to(jnp.sum(q[rows, :], axis=1, keepdims=True) * scale, (sub, LANES))
            acc = jnp.zeros((8, LANES), jnp.float32)
            for g in range(groups):
                v = z[g // 2, rows, pl.ds((g % 2) * LANES, LANES)]
                target = dense[pl.ds(r * (groups + 1) + g, sub, stride=groups + 1), :]
                dz[rows, pl.ds(g * LANES, LANES)] = (jnp.exp(v - lz) * s - target).astype(jnp.bfloat16)
                acc += jnp.sum((target * v).reshape(sub // 8, 8, LANES), axis=0)
            loss_acc[...] += acc
            slz_acc[...] += jnp.sum((s * lz).reshape(sub // 8, 8, LANES), axis=0)

        put_dz(c).start()
        part[c] = jnp.dot(dz[pl.ds(first, CHUNK), :], emb[...], preferred_element_type=jnp.float32)
        rdma(c, K_SIB).start()

        @pl.when(c < chunks - 1)
        def _():
            prepare(c + 1)
            build_targets(lo_s, code_s, (qh_s, qm_s, ql_s), dense, CHUNK, groups)

    def part_rows(first, count):
        return pl.ds(pl.multiple_of(first, 8), count)

    def stage_a(c):
        rdma(c, K_SIB).wait_recv()
        rows = part_rows(mine, half)
        part[c, rows, :] += sib_buf[c]
        for kind in (K_FAR_R, K_FAR_L, K_NEAR_R, K_NEAR_L):
            rdma(c, kind).start()

    def stage_b(c):
        rdma(c, K_FAR_R).wait_recv()
        part[c, part_rows(at(mine, right), bit), :] += ring_buf[c, 0]
        rdma(c, K_SUM_R).start()
        rdma(c, K_FAR_L).wait_recv()
        part[c, part_rows(at(mine, left, bit), bit), :] += ring_buf[c, 1]
        rdma(c, K_SUM_L).start()

    def stage_c(c):
        for kind in (K_NEAR_R, K_NEAR_L, K_SUM_R, K_SUM_L):
            rdma(c, kind).wait_recv()
        dx = part[c, part_rows(at(mine, chip), own), :] + jnp.concatenate(
            [ring_buf[c, K_SUM_R - 1] + ring_buf[c, K_NEAR_L - 1], ring_buf[c, K_SUM_L - 1] + ring_buf[c, K_NEAR_R - 1]], axis=0)
        h = hid[pl.ds(pl.multiple_of(c * CHUNK + at(mine, chip), own), own), :].astype(jnp.float32)
        inv = lax.rsqrt(jnp.mean(h * h, axis=1, keepdims=True) + 1e-6)
        unit = h * inv
        dy = dx * gain
        grad[c, part_rows(at(mine, chip), own), :] = inv * (dy - unit * jnp.mean(dy * unit, axis=1, keepdims=True))
        dw_acc[...] += jnp.sum((dx * unit).reshape(own // 8, 8, width), axis=0)
        for kind in (K_OUT_R, K_OUT_L, K_OUT_S):
            rdma(c, kind).start()

        @pl.when(c == chunks - 1)
        def _():
            dw = jnp.sum(dw_acc[...], axis=0, keepdims=True)
            for i in range(width // LANES):
                fin_buf[me, pl.ds(i, 1), :] = dw[:, i * LANES:(i + 1) * LANES]
            fin_buf[me, pl.ds(width // LANES, 1), :] = jnp.sum(loss_acc[...], axis=0, keepdims=True)
            for d in range(1, n_tp):
                everyone(fin_buf, fin_send, fin_recv, d).start()

    def stage_d(c):
        rdma(c, K_OUT_R).wait_recv()
        rdma(c, K_PASS_R).start()
        rdma(c, K_FWD_L).start()
        rdma(c, K_OUT_L).wait_recv()
        rdma(c, K_PASS_L).start()
        rdma(c, K_FWD_R).start()

    def stage_e(c):
        rdma(c, K_PASS_R).wait_recv()
        rdma(c, K_PASS_L).wait_recv()
        rdma(c, K_FWD_O).start()

    def stage_f(c):
        for kind in (K_OUT_S, K_FWD_L, K_FWD_R, K_FWD_O):
            rdma(c, kind).wait_recv()
        dh_s[pl.ds(pl.multiple_of(c * CHUNK, CHUNK), CHUNK), :] = grad[c].astype(jnp.bfloat16)
        put_dh(c).start()

    stages = ((LAG_F, stage_f), (LAG_E, stage_e), (LAG_D, stage_d), (LAG_C, stage_c), (LAG_B, stage_b), (LAG_A, stage_a), (0, compute))

    @pl.loop(0, chunks + LAG_F)
    def _(step):
        for lag, stage in stages:
            c = step - lag

            @pl.when((c >= 0) & (c < chunks))
            def _(c=c, stage=stage):
                stage(c)

    for d in range(1, n_tp):
        everyone(fin_buf, fin_send, fin_recv, d).wait_recv()
    fin = functools.reduce(jnp.add, [fin_buf[k] for k in range(n_tp)])
    lanes = width // LANES
    loss = jnp.sum(slz_acc[:, 0:1], axis=0, keepdims=True) - jnp.sum(fin[lanes:lanes + 1, :], axis=1, keepdims=True)
    fin_ref[...] = fin
    fin_ref[pl.ds(lanes, 1), :] = jnp.broadcast_to(loss, (1, LANES))

    for d in range(1, n_tp):
        everyone(stat_buf, stat_send, stat_recv, d).wait_send()
        everyone(fin_buf, fin_send, fin_recv, d).wait_send()

    @pl.loop(0, chunks)
    def _(c):
        for kind in range(KINDS):
            rdma(c, kind).wait_send()
        put_dz(c).wait()
        put_dh(c).wait()

    put_x.wait()


def solution(mesh):
    n_tp = mesh.shape['tp']

    def local_step(hidden, norm_gain, emb_block, teacher_ids, teacher_q):
        tokens, width = hidden.shape
        vocab = emb_block.shape[0]
        count = teacher_ids.shape[1]
        chunks = tokens // CHUNK
        half = CHUNK // 2
        bit = half // (n_tp // 2) // 2
        f32, bf16 = jnp.float32, jnp.bfloat16
        dma = pltpu.SemaphoreType.DMA
        hbm, vmem = pl.BlockSpec(memory_space=pl.ANY), pl.BlockSpec(memory_space=pltpu.VMEM)
        dh, x_in, grad_z, fin = pl.pallas_call(
            functools.partial(kernel, n_tp),
            out_shape=(jax.ShapeDtypeStruct((tokens, width), bf16), jax.ShapeDtypeStruct((tokens, width), bf16),
                       jax.ShapeDtypeStruct((tokens, vocab), bf16), jax.ShapeDtypeStruct((16, LANES), f32)),
            in_specs=[hbm, vmem, hbm, hbm, hbm],
            out_specs=(hbm, hbm, hbm, vmem),
            scratch_shapes=[
                pltpu.VMEM((tokens, width), bf16), pltpu.VMEM((vocab, width), bf16), pltpu.VMEM((tokens, count), jnp.int32), pltpu.VMEM((tokens, count), f32),
                pltpu.VMEM((tokens, width), bf16), pltpu.VMEM((vocab // BLOCK, tokens, BLOCK), f32), pltpu.VMEM((tokens, vocab), bf16), pltpu.VMEM((tokens, LANES), f32),
                *[pltpu.VMEM((CHUNK, count), f32)] * 5, pltpu.VMEM((CHUNK * (vocab // LANES + 1), LANES), f32),
                pltpu.VMEM((chunks, CHUNK, width), f32), pltpu.VMEM((chunks, half, width), f32), pltpu.VMEM((chunks, 6, bit, width), f32),
                pltpu.VMEM((chunks, CHUNK, width), f32), pltpu.VMEM((tokens, width), bf16),
                pltpu.VMEM((8, width), f32), pltpu.VMEM((8, LANES), f32), pltpu.VMEM((8, LANES), f32),
                pltpu.VMEM((n_tp, 2 * tokens // LANES, LANES), f32), pltpu.VMEM((n_tp, 16, LANES), f32),
                dma((3,)), dma((vocab // BLOCK,)), dma((chunks,)), dma((chunks,)), dma(()),
                dma((n_tp - 1,)), dma((n_tp - 1,)), dma((n_tp - 1,)), dma((n_tp - 1,)), dma((chunks, KINDS)), dma((chunks, KINDS)),
            ],
            compiler_params=pltpu.CompilerParams(collective_id=0, has_side_effects=True, vmem_limit_bytes=60 * 2**20),
        )(hidden, norm_gain[None, :], emb_block, teacher_ids, teacher_q)
        grad_block = lax.dot_general(grad_z, x_in, (((0,), (0,)), ((), ())), preferred_element_type=f32)
        lanes = width // LANES
        return fin[lanes, :1], dh, fin[:lanes].reshape(-1), grad_block

    return jax.shard_map(local_step, mesh=mesh, in_specs=(P('dp', None), P(None), P('tp', None), P('dp', None), P('dp', None)), out_specs=(P('dp'), P('dp', None), P('dp'), P(('dp', 'tp'), None)), check_vma=False)
```

```python
import functools

import jax
import jax.numpy as jnp
from jax import lax
from jax.experimental import pallas as pl
from jax.experimental.pallas import tpu as pltpu
from jax.sharding import PartitionSpec as P

LANES = 128
CHUNK = 128
BLOCK = 256
UNROLL = 32
MESH = pl.DeviceIdType.MESH
SLOTS = 3
LAG_A, LAG_B, LAG_C, LAG_D, LAG_E, LAG_F = 2, 6, 10, 14, 17, 18
(K_SIB, K_FAR_R, K_FAR_L, K_NEAR_R, K_NEAR_L, K_SUM_R, K_SUM_L, K_OUT_R, K_OUT_L, K_OUT_S,
 K_PASS_R, K_PASS_L, K_FWD_L, K_FWD_R, K_FWD_O) = range(15)
KINDS = 15


def build_targets(lo_ref, code_ref, pieces, dense_ref, first, tokens, groups):
    count = lo_ref.shape[1]
    sub, half = 16, LANES // 2
    base = lax.broadcasted_iota(jnp.int32, (sub, count), 0).astype(jnp.float32).astype(jnp.bfloat16)
    zero = jnp.zeros((sub, count), jnp.bfloat16)
    one = jnp.ones((sub, count), jnp.bfloat16)

    def row(ref, n):
        return jnp.broadcast_to(ref[pl.ds(n, 1), :], (sub, count)).astype(jnp.bfloat16)

    def one_token(n):
        lo, code = row(lo_ref, n), row(code_ref, n)
        weights = [row(ref, n) for ref in pieces]
        low_hot = jnp.concatenate([jnp.where(lo == base + jnp.bfloat16(sub * k), one, zero) for k in range(half // sub)], axis=0)
        here = [code == base + jnp.bfloat16(sub * k) for k in range(2 * groups // sub)]
        lhs = jnp.concatenate([jnp.where(h, w, zero) for w in weights for h in here], axis=0)
        out = lax.dot_general(lhs, low_hot, (((1,), (1,)), ((), ())), preferred_element_type=jnp.float32)
        out = out[:2 * groups] + out[2 * groups:4 * groups] + out[4 * groups:]
        dense_ref[pl.ds(n * (groups + 1), groups), :] = jnp.concatenate([out[:groups], out[groups:]], axis=1)

    @pl.loop(0, tokens // UNROLL)
    def _(i):
        for u in range(UNROLL):
            one_token(first + i * UNROLL + u)


def kernel(n_tp, hid_hbm, gain_ref, emb_hbm, ids_hbm, q_hbm, dh_hbm, x_hbm, dz_hbm, fin_ref,
           hid, emb, ids, q, xs, z, dz, lz_s, lo_s, code_s, qh_s, qm_s, ql_s, dense, part, sib_buf, ring_buf,
           grad, dh_s, dw_acc, loss_acc, slz_acc, stat_buf, fin_buf,
           in_sem, emb_sem, out_sem, dh_sem, x_sem, stat_send, stat_recv, fin_send, fin_recv, send_sem, recv_sem):
    tokens, width = hid.shape
    vocab = emb.shape[0]
    groups = vocab // LANES
    chunks = tokens // CHUNK
    chips = n_tp // 2
    half = CHUNK // 2
    own = half // chips
    bit = own // 2
    scale = 1.0 / tokens
    dp, me = lax.axis_index('dp'), lax.axis_index('tp')
    core = lax.rem(me, 2)
    chip = me // 2
    right = lax.rem(chip + 1, chips)
    left = lax.rem(chip + chips - 1, chips)
    far = lax.rem(chip + 2, chips)
    to_right, to_left, to_sib = right * 2 + core, left * 2 + core, chip * 2 + 1 - core

    barrier = pltpu.get_barrier_semaphore()
    for d in range(1, n_tp):
        pl.semaphore_signal(barrier, inc=1, device_id=(dp, lax.rem(me + d, n_tp)), device_id_type=MESH)

    get_hid = pltpu.make_async_copy(hid_hbm, hid, in_sem.at[0])
    get_ids = pltpu.make_async_copy(ids_hbm, ids, in_sem.at[1])
    get_q = pltpu.make_async_copy(q_hbm, q, in_sem.at[2])

    def get_emb(b):
        rows = pl.ds(pl.multiple_of(b * BLOCK, BLOCK), BLOCK)
        return pltpu.make_async_copy(emb_hbm.at[rows], emb.at[rows], emb_sem.at[b])

    get_hid.start()
    for b in range(vocab // BLOCK):
        get_emb(b).start()
    get_ids.start()
    get_q.start()

    get_hid.wait()
    gain = 1.0 + gain_ref[...].reshape(1, width)

    @pl.loop(0, tokens // 32)
    def _(i):
        rows = pl.ds(pl.multiple_of(i * 32, 32), 32)
        h = hid[rows, :].astype(jnp.float32)
        inv = lax.rsqrt(jnp.mean(h * h, axis=1, keepdims=True) + 1e-6)
        xs[rows, :] = (h * inv * gain).astype(jnp.bfloat16)

    put_x = pltpu.make_async_copy(xs, x_hbm, x_sem)
    put_x.start()

    @pl.loop(0, vocab // BLOCK)
    def _(b):
        get_emb(b).wait()
        rows = pl.ds(pl.multiple_of(b * BLOCK, BLOCK), BLOCK)
        for r in range(0, tokens, min(512, tokens)):
            z[b, pl.ds(r, min(512, tokens)), :] = lax.dot_general(xs[pl.ds(r, min(512, tokens)), :], emb[rows, :], (((1,), (1,)), ((), ())), preferred_element_type=jnp.float32)

    eye = lax.broadcasted_iota(jnp.int32, (LANES, LANES), 0) == lax.broadcasted_iota(jnp.int32, (LANES, LANES), 1)

    def as_row(tile):
        return jnp.sum(jnp.where(eye, tile, 0.0), axis=0, keepdims=True)

    stat_rows = tokens // LANES

    @pl.loop(0, stat_rows)
    def _(t):
        for u in range(0, LANES, 32):
            rows = pl.ds(pl.multiple_of(t * LANES + u, 32), 32)
            tiles = [z[g // 2, rows, pl.ds((g % 2) * LANES, LANES)] for g in range(groups)]
            peak = functools.reduce(jnp.maximum, tiles)
            peak = jnp.broadcast_to(jnp.max(peak, axis=1, keepdims=True), (32, LANES))
            total = functools.reduce(jnp.add, [jnp.exp(v - peak) for v in tiles])
            lz_s[rows, :] = peak
            dense[pl.ds(u, 32), :] = jnp.broadcast_to(jnp.sum(total, axis=1, keepdims=True), (32, LANES))
        stat_buf[me, pl.ds(t, 1), :] = as_row(lz_s[pl.ds(pl.multiple_of(t * LANES, LANES), LANES), :])
        stat_buf[me, pl.ds(stat_rows + t, 1), :] = as_row(dense[pl.ds(0, LANES), :])

    def everyone(buf, send, recv, d):
        return pltpu.make_async_remote_copy(
            src_ref=buf.at[me], dst_ref=buf.at[me], send_sem=send.at[d - 1], recv_sem=recv.at[d - 1],
            device_id=(dp, lax.rem(me + d, n_tp)), device_id_type=MESH)

    pl.semaphore_wait(barrier, n_tp - 1)
    for d in range(1, n_tp):
        everyone(stat_buf, stat_send, stat_recv, d).start()

    get_ids.wait()
    get_q.wait()
    start = me * vocab

    def prepare(c):
        @pl.loop(0, CHUNK // 32)
        def _(i):
            rows = pl.ds(pl.multiple_of(i * 32, 32), 32)
            src = pl.ds(pl.multiple_of(c * CHUNK + i * 32, 32), 32)
            lid = ids[src, :] - start
            lo_s[rows, :] = jnp.bitwise_and(lid, LANES // 2 - 1).astype(jnp.float32)
            code = jnp.right_shift(lid, 7) + groups * jnp.bitwise_and(jnp.right_shift(lid, 6), 1)
            code_s[rows, :] = jnp.where((lid >= 0) & (lid < vocab), code, -1).astype(jnp.float32)
            w = q[src, :] * scale
            wh = w.astype(jnp.bfloat16).astype(jnp.float32)
            rest = w - wh
            wm = rest.astype(jnp.bfloat16).astype(jnp.float32)
            qh_s[rows, :] = wh
            qm_s[rows, :] = wm
            ql_s[rows, :] = rest - wm

    prepare(0)
    build_targets(lo_s, code_s, (qh_s, qm_s, ql_s), dense, 0, CHUNK, groups)

    for d in range(1, n_tp):
        everyone(stat_buf, stat_send, stat_recv, d).wait_recv()
    peaks = [stat_buf[k, pl.ds(0, stat_rows), :] for k in range(n_tp)]
    peak = functools.reduce(jnp.maximum, peaks)
    total = functools.reduce(jnp.add, [stat_buf[k, pl.ds(stat_rows, stat_rows), :] * jnp.exp(peaks[k] - peak) for k in range(n_tp)])
    log_z = peak + jnp.log(total)
    for t in range(stat_rows):
        tile = jnp.where(eye, jnp.broadcast_to(log_z[t:t + 1, :], (LANES, LANES)), 0.0)
        lz_s[pl.ds(t * LANES, LANES), :] = jnp.broadcast_to(jnp.sum(tile, axis=1, keepdims=True), (LANES, LANES))

    fin_buf[me] = jnp.zeros(fin_buf.shape[1:], jnp.float32)
    dw_acc[...] = jnp.zeros_like(dw_acc)
    loss_acc[...] = jnp.zeros_like(loss_acc)
    slz_acc[...] = jnp.zeros_like(slz_acc)

    mine = core * half
    theirs = half - mine

    def at(base, block, off=0):
        return base + block * own + off

    def rdma(c, kind):
        def rows(first, count):
            return pl.ds(pl.multiple_of(first, 8), count)

        if kind == K_SIB:
            src, dst, peer = part.at[c, rows(theirs, half)], sib_buf.at[c], to_sib
        elif kind in (K_FAR_R, K_FAR_L, K_NEAR_R, K_NEAR_L, K_SUM_R, K_SUM_L):
            first = {K_FAR_R: at(mine, far), K_FAR_L: at(mine, far, bit), K_NEAR_R: at(mine, right, bit),
                     K_NEAR_L: at(mine, left), K_SUM_R: at(mine, right), K_SUM_L: at(mine, left, bit)}[kind]
            src, dst = part.at[c, rows(first, bit)], ring_buf.at[c, kind - K_FAR_R]
            peer = to_right if kind in (K_FAR_R, K_NEAR_R, K_SUM_R) else to_left
        else:
            first, count, peer = {
                K_OUT_R: (at(mine, chip), own, to_right), K_OUT_L: (at(mine, chip), own, to_left), K_OUT_S: (at(mine, chip), own, to_sib),
                K_PASS_R: (at(mine, left), bit, to_right), K_PASS_L: (at(mine, right, bit), bit, to_left),
                K_FWD_L: (at(mine, left), own, to_sib), K_FWD_R: (at(mine, right), own, to_sib), K_FWD_O: (at(mine, far), own, to_sib)}[kind]
            src = dst = grad.at[c, rows(first, count)]
        return pltpu.make_async_remote_copy(src_ref=src, dst_ref=dst, send_sem=send_sem.at[c, kind], recv_sem=recv_sem.at[c, kind],
                                            device_id=(dp, peer), device_id_type=MESH)

    def put_dz(c):
        rows = pl.ds(pl.multiple_of(c * CHUNK, CHUNK), CHUNK)
        return pltpu.make_async_copy(dz.at[rows], dz_hbm.at[rows], out_sem.at[c])

    def put_dh(c):
        rows = pl.ds(pl.multiple_of(c * CHUNK, CHUNK), CHUNK)
        return pltpu.make_async_copy(dh_s.at[rows], dh_hbm.at[rows], dh_sem.at[c])

    def compute(c):
        sub = 32
        first = pl.multiple_of(c * CHUNK, CHUNK)

        @pl.loop(0, CHUNK // sub)
        def _(i):
            r = pl.multiple_of(i * sub, sub)
            rows = pl.ds(pl.multiple_of(first + r, sub), sub)
            lz = lz_s[rows, :]
            s = jnp.broadcast_to(jnp.sum(q[rows, :], axis=1, keepdims=True) * scale, (sub, LANES))
            acc = jnp.zeros((8, LANES), jnp.float32)
            for g in range(groups):
                v = z[g // 2, rows, pl.ds((g % 2) * LANES, LANES)]
                target = dense[pl.ds(r * (groups + 1) + g, sub, stride=groups + 1), :]
                dz[rows, pl.ds(g * LANES, LANES)] = (jnp.exp(v - lz) * s - target).astype(jnp.bfloat16)
                acc += jnp.sum((target * v).reshape(sub // 8, 8, LANES), axis=0)
            loss_acc[...] += acc
            slz_acc[...] += jnp.sum((s * lz).reshape(sub // 8, 8, LANES), axis=0)

        put_dz(c).start()
        part[c] = jnp.dot(dz[pl.ds(first, CHUNK), :], emb[...], preferred_element_type=jnp.float32)
        rdma(c, K_SIB).start()

    def part_rows(first, count):
        return pl.ds(pl.multiple_of(first, 8), count)

    def stage_a(c):
        rdma(c, K_SIB).wait_recv()
        rows = part_rows(mine, half)
        part[c, rows, :] += sib_buf[c]
        for kind in (K_FAR_R, K_FAR_L, K_NEAR_R, K_NEAR_L):
            rdma(c, kind).start()

    def stage_b(c):
        rdma(c, K_FAR_R).wait_recv()
        part[c, part_rows(at(mine, right), bit), :] += ring_buf[c, 0]
        rdma(c, K_SUM_R).start()
        rdma(c, K_FAR_L).wait_recv()
        part[c, part_rows(at(mine, left, bit), bit), :] += ring_buf[c, 1]
        rdma(c, K_SUM_L).start()

    def stage_c(c):
        for kind in (K_NEAR_R, K_NEAR_L, K_SUM_R, K_SUM_L):
            rdma(c, kind).wait_recv()
        dx = part[c, part_rows(at(mine, chip), own), :] + jnp.concatenate(
            [ring_buf[c, K_SUM_R - 1] + ring_buf[c, K_NEAR_L - 1], ring_buf[c, K_SUM_L - 1] + ring_buf[c, K_NEAR_R - 1]], axis=0)
        h = hid[pl.ds(pl.multiple_of(c * CHUNK + at(mine, chip), own), own), :].astype(jnp.float32)
        inv = lax.rsqrt(jnp.mean(h * h, axis=1, keepdims=True) + 1e-6)
        unit = h * inv
        dy = dx * gain
        grad[c, part_rows(at(mine, chip), own), :] = inv * (dy - unit * jnp.mean(dy * unit, axis=1, keepdims=True))
        dw_acc[...] += jnp.sum((dx * unit).reshape(own // 8, 8, width), axis=0)
        for kind in (K_OUT_R, K_OUT_L, K_OUT_S):
            rdma(c, kind).start()

        @pl.when(c == chunks - 1)
        def _():
            dw = jnp.sum(dw_acc[...], axis=0, keepdims=True)
            for i in range(width // LANES):
                fin_buf[me, pl.ds(i, 1), :] = dw[:, i * LANES:(i + 1) * LANES]
            fin_buf[me, pl.ds(width // LANES, 1), :] = jnp.sum(loss_acc[...], axis=0, keepdims=True)
            for d in range(1, n_tp):
                everyone(fin_buf, fin_send, fin_recv, d).start()

    def stage_d(c):
        rdma(c, K_OUT_R).wait_recv()
        rdma(c, K_PASS_R).start()
        rdma(c, K_FWD_L).start()
        rdma(c, K_OUT_L).wait_recv()
        rdma(c, K_PASS_L).start()
        rdma(c, K_FWD_R).start()

    def stage_e(c):
        rdma(c, K_PASS_R).wait_recv()
        rdma(c, K_PASS_L).wait_recv()
        rdma(c, K_FWD_O).start()

    def stage_f(c):
        for kind in (K_OUT_S, K_FWD_L, K_FWD_R, K_FWD_O):
            rdma(c, kind).wait_recv()
        dh_s[pl.ds(pl.multiple_of(c * CHUNK, CHUNK), CHUNK), :] = grad[c].astype(jnp.bfloat16)
        put_dh(c).start()

    stages = ((LAG_F, stage_f), (LAG_E, stage_e), (LAG_D, stage_d), (LAG_C, stage_c), (LAG_B, stage_b), (LAG_A, stage_a), (0, compute))

    @pl.loop(0, SLOTS * chunks + LAG_F - SLOTS + 1)
    def _(slot):
        for lag, stage in stages:
            since = slot - lag

            @pl.when((since >= 0) & (lax.rem(since + SLOTS * LAG_F, SLOTS) == 0) & (since < SLOTS * chunks))
            def _(since=since, stage=stage):
                stage(since // SLOTS)

        phase = lax.rem(slot, SLOTS)
        c = slot // SLOTS

        @pl.when((phase == 1) & (c < chunks - 1))
        def _():
            prepare(c + 1)

        @pl.when((phase >= 1) & (c < chunks - 1))
        def _():
            build_targets(lo_s, code_s, (qh_s, qm_s, ql_s), dense, (phase - 1) * (CHUNK // 2), CHUNK // 2, groups)

    for d in range(1, n_tp):
        everyone(fin_buf, fin_send, fin_recv, d).wait_recv()
    fin = functools.reduce(jnp.add, [fin_buf[k] for k in range(n_tp)])
    lanes = width // LANES
    loss = jnp.sum(slz_acc[:, 0:1], axis=0, keepdims=True) - jnp.sum(fin[lanes:lanes + 1, :], axis=1, keepdims=True)
    fin_ref[...] = fin
    fin_ref[pl.ds(lanes, 1), :] = jnp.broadcast_to(loss, (1, LANES))

    for d in range(1, n_tp):
        everyone(stat_buf, stat_send, stat_recv, d).wait_send()
        everyone(fin_buf, fin_send, fin_recv, d).wait_send()

    @pl.loop(0, chunks)
    def _(c):
        for kind in range(KINDS):
            rdma(c, kind).wait_send()
        put_dz(c).wait()
        put_dh(c).wait()

    put_x.wait()


def solution(mesh):
    n_tp = mesh.shape['tp']

    def local_step(hidden, norm_gain, emb_block, teacher_ids, teacher_q):
        tokens, width = hidden.shape
        vocab = emb_block.shape[0]
        count = teacher_ids.shape[1]
        chunks = tokens // CHUNK
        half = CHUNK // 2
        bit = half // (n_tp // 2) // 2
        f32, bf16 = jnp.float32, jnp.bfloat16
        dma = pltpu.SemaphoreType.DMA
        hbm, vmem = pl.BlockSpec(memory_space=pl.ANY), pl.BlockSpec(memory_space=pltpu.VMEM)
        dh, x_in, grad_z, fin = pl.pallas_call(
            functools.partial(kernel, n_tp),
            out_shape=(jax.ShapeDtypeStruct((tokens, width), bf16), jax.ShapeDtypeStruct((tokens, width), bf16),
                       jax.ShapeDtypeStruct((tokens, vocab), bf16), jax.ShapeDtypeStruct((16, LANES), f32)),
            in_specs=[hbm, vmem, hbm, hbm, hbm],
            out_specs=(hbm, hbm, hbm, vmem),
            scratch_shapes=[
                pltpu.VMEM((tokens, width), bf16), pltpu.VMEM((vocab, width), bf16), pltpu.VMEM((tokens, count), jnp.int32), pltpu.VMEM((tokens, count), f32),
                pltpu.VMEM((tokens, width), bf16), pltpu.VMEM((vocab // BLOCK, tokens, BLOCK), f32), pltpu.VMEM((tokens, vocab), bf16), pltpu.VMEM((tokens, LANES), f32),
                *[pltpu.VMEM((CHUNK, count), f32)] * 5, pltpu.VMEM((CHUNK * (vocab // LANES + 1), LANES), f32),
                pltpu.VMEM((chunks, CHUNK, width), f32), pltpu.VMEM((chunks, half, width), f32), pltpu.VMEM((chunks, 6, bit, width), f32),
                pltpu.VMEM((chunks, CHUNK, width), f32), pltpu.VMEM((tokens, width), bf16),
                pltpu.VMEM((8, width), f32), pltpu.VMEM((8, LANES), f32), pltpu.VMEM((8, LANES), f32),
                pltpu.VMEM((n_tp, 2 * tokens // LANES, LANES), f32), pltpu.VMEM((n_tp, 16, LANES), f32),
                dma((3,)), dma((vocab // BLOCK,)), dma((chunks,)), dma((chunks,)), dma(()),
                dma((n_tp - 1,)), dma((n_tp - 1,)), dma((n_tp - 1,)), dma((n_tp - 1,)), dma((chunks, KINDS)), dma((chunks, KINDS)),
            ],
            compiler_params=pltpu.CompilerParams(collective_id=0, has_side_effects=True, vmem_limit_bytes=60 * 2**20),
        )(hidden, norm_gain, emb_block, teacher_ids, teacher_q)
        grad_block = lax.dot_general(grad_z, x_in, (((0,), (0,)), ((), ())), preferred_element_type=f32)
        lanes = width // LANES
        return fin[lanes, :1], dh, fin[:lanes].reshape(-1), grad_block

    return jax.shard_map(local_step, mesh=mesh, in_specs=(P('dp', None), P(None), P('tp', None), P('dp', None), P('dp', None)), out_specs=(P('dp'), P('dp', None), P('dp'), P(('dp', 'tp'), None)), check_vma=False)
```

```python
import functools

import jax
import jax.numpy as jnp
from jax import lax
from jax.experimental import pallas as pl
from jax.experimental.pallas import tpu as pltpu
from jax.sharding import PartitionSpec as P

LANES = 128
CHUNK = 128
BLOCK = 256
SUB = 32
MESH = pl.DeviceIdType.MESH
SLOTS = 3
LAG_A, LAG_B, LAG_C, LAG_D, LAG_E, LAG_F = 2, 6, 10, 14, 17, 18
(K_SIB, K_FAR_R, K_FAR_L, K_NEAR_R, K_NEAR_L, K_SUM_R, K_SUM_L, K_OUT_R, K_OUT_L, K_OUT_S,
 K_PASS_R, K_PASS_L, K_FWD_L, K_FWD_R, K_FWD_O) = range(15)
KINDS = 15


def build_targets(lo_ref, code_ref, pieces, dense_ref, first, tokens, groups):
    count = lo_ref.shape[1]
    sub, half = 16, LANES // 2
    base = lax.broadcasted_iota(jnp.int32, (sub, count), 0).astype(jnp.float32).astype(jnp.bfloat16)
    zero = jnp.zeros((sub, count), jnp.bfloat16)
    one = jnp.ones((sub, count), jnp.bfloat16)

    def row(ref, n):
        return jnp.broadcast_to(ref[pl.ds(n, 1), :], (sub, count)).astype(jnp.bfloat16)

    def one_token(n):
        lo, code = row(lo_ref, n), row(code_ref, n)
        weights = [row(ref, n) for ref in pieces]
        low_hot = jnp.concatenate([jnp.where(lo == base + jnp.bfloat16(sub * k), one, zero) for k in range(half // sub)], axis=0)
        here = [code == base + jnp.bfloat16(sub * k) for k in range(2 * groups // sub)]
        lhs = jnp.concatenate([jnp.where(h, w, zero) for w in weights for h in here], axis=0)
        out = lax.dot_general(lhs, low_hot, (((1,), (1,)), ((), ())), preferred_element_type=jnp.float32)
        out = out[:2 * groups] + out[2 * groups:4 * groups] + out[4 * groups:]
        dense_ref[pl.ds(n * (groups + 1), groups), :] = jnp.concatenate([out[:groups], out[groups:]], axis=1)

    for u in range(tokens):
        one_token(first + u)


def kernel(n_tp, hid_hbm, gain_ref, emb_hbm, ids_hbm, q_hbm, dh_hbm, de_hbm, fin_ref,
           hid, emb, ids, q, xs, z, dz, lz_s, lo_s, code_s, qh_s, qm_s, ql_s, dense, part, sib_buf, ring_buf,
           grad, dh_s, de_buf, dw_acc, loss_acc, slz_acc, stat_buf, fin_buf,
           in_sem, emb_sem, de_sem, dh_sem, stat_send, stat_recv, fin_send, fin_recv, send_sem, recv_sem):
    tokens, width = hid.shape
    vocab = emb.shape[0]
    groups = vocab // LANES
    chunks = tokens // CHUNK
    chips = n_tp // 2
    half = CHUNK // 2
    own = half // chips
    bit = own // 2
    scale = 1.0 / tokens
    dp, me = lax.axis_index('dp'), lax.axis_index('tp')
    core = lax.rem(me, 2)
    chip = me // 2
    right = lax.rem(chip + 1, chips)
    left = lax.rem(chip + chips - 1, chips)
    far = lax.rem(chip + 2, chips)
    to_right, to_left, to_sib = right * 2 + core, left * 2 + core, chip * 2 + 1 - core

    barrier = pltpu.get_barrier_semaphore()
    for d in range(1, n_tp):
        pl.semaphore_signal(barrier, inc=1, device_id=(dp, lax.rem(me + d, n_tp)), device_id_type=MESH)

    get_hid = pltpu.make_async_copy(hid_hbm, hid, in_sem.at[0])
    get_ids = pltpu.make_async_copy(ids_hbm, ids, in_sem.at[1])
    get_q = pltpu.make_async_copy(q_hbm, q, in_sem.at[2])

    def get_emb(b):
        rows = pl.ds(pl.multiple_of(b * BLOCK, BLOCK), BLOCK)
        return pltpu.make_async_copy(emb_hbm.at[rows], emb.at[rows], emb_sem.at[b])

    get_hid.start()
    for b in range(vocab // BLOCK):
        get_emb(b).start()
    get_ids.start()
    get_q.start()

    get_hid.wait()
    gain = 1.0 + gain_ref[...].reshape(1, width)

    @pl.loop(0, tokens // 32)
    def _(i):
        rows = pl.ds(pl.multiple_of(i * 32, 32), 32)
        h = hid[rows, :].astype(jnp.float32)
        inv = lax.rsqrt(jnp.mean(h * h, axis=1, keepdims=True) + 1e-6)
        xs[rows, :] = (h * inv * gain).astype(jnp.bfloat16)

    @pl.loop(0, vocab // BLOCK)
    def _(b):
        get_emb(b).wait()
        rows = pl.ds(pl.multiple_of(b * BLOCK, BLOCK), BLOCK)
        z[b] = lax.dot_general(xs[...], emb[rows, :], (((1,), (1,)), ((), ())), preferred_element_type=jnp.float32)

    eye = lax.broadcasted_iota(jnp.int32, (LANES, LANES), 0) == lax.broadcasted_iota(jnp.int32, (LANES, LANES), 1)

    def as_row(tile):
        return jnp.sum(jnp.where(eye, tile, 0.0), axis=0, keepdims=True)

    stat_rows = tokens // LANES

    @pl.loop(0, stat_rows)
    def _(t):
        for u in range(0, LANES, 32):
            rows = pl.ds(pl.multiple_of(t * LANES + u, 32), 32)
            tiles = [z[g // 2, rows, pl.ds((g % 2) * LANES, LANES)] for g in range(groups)]
            peak = functools.reduce(jnp.maximum, tiles)
            peak = jnp.broadcast_to(jnp.max(peak, axis=1, keepdims=True), (32, LANES))
            total = functools.reduce(jnp.add, [jnp.exp(v - peak) for v in tiles])
            lz_s[rows, :] = peak
            dense[pl.ds(u, 32), :] = jnp.broadcast_to(jnp.sum(total, axis=1, keepdims=True), (32, LANES))
        stat_buf[me, pl.ds(t, 1), :] = as_row(lz_s[pl.ds(pl.multiple_of(t * LANES, LANES), LANES), :])
        stat_buf[me, pl.ds(stat_rows + t, 1), :] = as_row(dense[pl.ds(0, LANES), :])

    def everyone(buf, send, recv, d):
        return pltpu.make_async_remote_copy(
            src_ref=buf.at[me], dst_ref=buf.at[me], send_sem=send.at[d - 1], recv_sem=recv.at[d - 1],
            device_id=(dp, lax.rem(me + d, n_tp)), device_id_type=MESH)

    pl.semaphore_wait(barrier, n_tp - 1)
    for d in range(1, n_tp):
        everyone(stat_buf, stat_send, stat_recv, d).start()

    get_ids.wait()
    get_q.wait()
    start = me * vocab

    def prepare(c):
        @pl.loop(0, CHUNK // 32)
        def _(i):
            rows = pl.ds(pl.multiple_of(i * 32, 32), 32)
            src = pl.ds(pl.multiple_of(c * CHUNK + i * 32, 32), 32)
            lid = ids[src, :] - start
            lo_s[rows, :] = jnp.bitwise_and(lid, LANES // 2 - 1).astype(jnp.float32)
            code = jnp.right_shift(lid, 7) + groups * jnp.bitwise_and(jnp.right_shift(lid, 6), 1)
            code_s[rows, :] = jnp.where((lid >= 0) & (lid < vocab), code, -1).astype(jnp.float32)
            w = q[src, :] * scale
            wh = w.astype(jnp.bfloat16).astype(jnp.float32)
            rest = w - wh
            wm = rest.astype(jnp.bfloat16).astype(jnp.float32)
            qh_s[rows, :] = wh
            qm_s[rows, :] = wm
            ql_s[rows, :] = rest - wm

    blocks = CHUNK // SUB

    def targets(i):
        build_targets(lo_s, code_s, (qh_s, qm_s, ql_s), dense, i * SUB, SUB, groups)

    prepare(0)

    @pl.loop(0, blocks)
    def _(i):
        targets(i)

    for d in range(1, n_tp):
        everyone(stat_buf, stat_send, stat_recv, d).wait_recv()
    peaks = [stat_buf[k, pl.ds(0, stat_rows), :] for k in range(n_tp)]
    peak = functools.reduce(jnp.maximum, peaks)
    total = functools.reduce(jnp.add, [stat_buf[k, pl.ds(stat_rows, stat_rows), :] * jnp.exp(peaks[k] - peak) for k in range(n_tp)])
    log_z = peak + jnp.log(total)
    for t in range(stat_rows):
        tile = jnp.where(eye, jnp.broadcast_to(log_z[t:t + 1, :], (LANES, LANES)), 0.0)
        lz_s[pl.ds(t * LANES, LANES), :] = jnp.broadcast_to(jnp.sum(tile, axis=1, keepdims=True), (LANES, LANES))

    fin_buf[me] = jnp.zeros(fin_buf.shape[1:], jnp.float32)
    dw_acc[...] = jnp.zeros_like(dw_acc)
    loss_acc[...] = jnp.zeros_like(loss_acc)
    slz_acc[...] = jnp.zeros_like(slz_acc)

    mine = core * half
    theirs = half - mine

    def at(base, block, off=0):
        return base + block * own + off

    def rdma(c, kind):
        def rows(first, count):
            return pl.ds(pl.multiple_of(first, 8), count)

        if kind == K_SIB:
            src, dst, peer = part.at[c, rows(theirs, half)], sib_buf.at[c], to_sib
        elif kind in (K_FAR_R, K_FAR_L, K_NEAR_R, K_NEAR_L, K_SUM_R, K_SUM_L):
            first = {K_FAR_R: at(mine, far), K_FAR_L: at(mine, far, bit), K_NEAR_R: at(mine, right, bit),
                     K_NEAR_L: at(mine, left), K_SUM_R: at(mine, right), K_SUM_L: at(mine, left, bit)}[kind]
            src, dst = part.at[c, rows(first, bit)], ring_buf.at[c, kind - K_FAR_R]
            peer = to_right if kind in (K_FAR_R, K_NEAR_R, K_SUM_R) else to_left
        else:
            first, count, peer = {
                K_OUT_R: (at(mine, chip), own, to_right), K_OUT_L: (at(mine, chip), own, to_left), K_OUT_S: (at(mine, chip), own, to_sib),
                K_PASS_R: (at(mine, left), bit, to_right), K_PASS_L: (at(mine, right, bit), bit, to_left),
                K_FWD_L: (at(mine, left), own, to_sib), K_FWD_R: (at(mine, right), own, to_sib), K_FWD_O: (at(mine, far), own, to_sib)}[kind]
            src = dst = grad.at[c, rows(first, count)]
        return pltpu.make_async_remote_copy(src_ref=src, dst_ref=dst, send_sem=send_sem.at[c, kind], recv_sem=recv_sem.at[c, kind],
                                            device_id=(dp, peer), device_id_type=MESH)

    def put_de(k):
        rows = pl.ds(pl.multiple_of(k * BLOCK, BLOCK), BLOCK)
        return pltpu.make_async_copy(de_buf.at[lax.rem(k, 2)], de_hbm.at[rows], de_sem.at[k])

    def put_dh(c):
        rows = pl.ds(pl.multiple_of(c * CHUNK, CHUNK), CHUNK)
        return pltpu.make_async_copy(dh_s.at[rows], dh_hbm.at[rows], dh_sem.at[c])

    def make_dz(c, i):
        r = pl.multiple_of(i * SUB, SUB)
        rows = pl.ds(pl.multiple_of(c * CHUNK + r, SUB), SUB)
        lz = lz_s[rows, :]
        s = jnp.broadcast_to(jnp.sum(q[rows, :], axis=1, keepdims=True) * scale, (SUB, LANES))
        acc = jnp.zeros((8, LANES), jnp.float32)
        for g in range(groups):
            v = z[g // 2, rows, pl.ds((g % 2) * LANES, LANES)]
            target = dense[pl.ds(r * (groups + 1) + g, SUB, stride=groups + 1), :]
            dz[rows, pl.ds(g * LANES, LANES)] = (jnp.exp(v - lz) * s - target).astype(jnp.bfloat16)
            acc += jnp.sum((target * v).reshape(SUB // 8, 8, LANES), axis=0)
        loss_acc[...] += acc
        slz_acc[...] += jnp.sum((s * lz).reshape(SUB // 8, 8, LANES), axis=0)

    def make_dx(c):
        part[c] = jnp.dot(dz[pl.ds(pl.multiple_of(c * CHUNK, CHUNK), CHUNK), :], emb[...], preferred_element_type=jnp.float32)
        rdma(c, K_SIB).start()

    def make_de(k):
        @pl.when(k >= 2)
        def _():
            put_de(k - 2).wait()

        cols = pl.ds(pl.multiple_of(k * BLOCK, BLOCK), BLOCK)
        de_buf[lax.rem(k, 2)] = lax.dot_general(dz[:, cols], xs[...], (((0,), (0,)), ((), ())), preferred_element_type=jnp.float32)
        put_de(k).start()

    def part_rows(first, count):
        return pl.ds(pl.multiple_of(first, 8), count)

    def stage_a(c):
        rdma(c, K_SIB).wait_recv()
        rows = part_rows(mine, half)
        part[c, rows, :] += sib_buf[c]
        for kind in (K_FAR_R, K_FAR_L, K_NEAR_R, K_NEAR_L):
            rdma(c, kind).start()

    def stage_b(c):
        rdma(c, K_FAR_R).wait_recv()
        part[c, part_rows(at(mine, right), bit), :] += ring_buf[c, 0]
        rdma(c, K_SUM_R).start()
        rdma(c, K_FAR_L).wait_recv()
        part[c, part_rows(at(mine, left, bit), bit), :] += ring_buf[c, 1]
        rdma(c, K_SUM_L).start()

    def stage_c(c):
        for kind in (K_NEAR_R, K_NEAR_L, K_SUM_R, K_SUM_L):
            rdma(c, kind).wait_recv()
        dx = part[c, part_rows(at(mine, chip), own), :] + jnp.concatenate(
            [ring_buf[c, K_SUM_R - 1] + ring_buf[c, K_NEAR_L - 1], ring_buf[c, K_SUM_L - 1] + ring_buf[c, K_NEAR_R - 1]], axis=0)
        h = hid[pl.ds(pl.multiple_of(c * CHUNK + at(mine, chip), own), own), :].astype(jnp.float32)
        inv = lax.rsqrt(jnp.mean(h * h, axis=1, keepdims=True) + 1e-6)
        unit = h * inv
        dy = dx * gain
        grad[c, part_rows(at(mine, chip), own), :] = inv * (dy - unit * jnp.mean(dy * unit, axis=1, keepdims=True))
        dw_acc[...] += jnp.sum((dx * unit).reshape(own // 8, 8, width), axis=0)
        for kind in (K_OUT_R, K_OUT_L, K_OUT_S):
            rdma(c, kind).start()

        @pl.when(c == chunks - 1)
        def _():
            dw = jnp.sum(dw_acc[...], axis=0, keepdims=True)
            for i in range(width // LANES):
                fin_buf[me, pl.ds(i, 1), :] = dw[:, i * LANES:(i + 1) * LANES]
            fin_buf[me, pl.ds(width // LANES, 1), :] = jnp.sum(loss_acc[...], axis=0, keepdims=True)
            for d in range(1, n_tp):
                everyone(fin_buf, fin_send, fin_recv, d).start()

    def stage_d(c):
        rdma(c, K_OUT_R).wait_recv()
        rdma(c, K_PASS_R).start()
        rdma(c, K_FWD_L).start()
        rdma(c, K_OUT_L).wait_recv()
        rdma(c, K_PASS_L).start()
        rdma(c, K_FWD_R).start()

    def stage_e(c):
        rdma(c, K_PASS_R).wait_recv()
        rdma(c, K_PASS_L).wait_recv()
        rdma(c, K_FWD_O).start()

    def stage_f(c):
        for kind in (K_OUT_S, K_FWD_L, K_FWD_R, K_FWD_O):
            rdma(c, kind).wait_recv()
        dh_s[pl.ds(pl.multiple_of(c * CHUNK, CHUNK), CHUNK), :] = grad[c].astype(jnp.bfloat16)
        put_dh(c).start()

    stages = ((LAG_F, stage_f), (LAG_E, stage_e), (LAG_D, stage_d), (LAG_C, stage_c), (LAG_B, stage_b), (LAG_A, stage_a))

    @pl.loop(0, blocks - 1)
    def _(i):
        make_dz(0, i)

    de_blocks = vocab // BLOCK
    last = SLOTS * (chunks - 1)

    @pl.loop(0, SLOTS * chunks + LAG_F - SLOTS + 1)
    def _(slot):
        for lag, stage in stages:
            since = slot - lag

            @pl.when((since >= 0) & (lax.rem(since + SLOTS * LAG_F, SLOTS) == 0) & (since < SLOTS * chunks))
            def _(since=since, stage=stage):
                stage(since // SLOTS)

        phase = lax.rem(slot, SLOTS)
        c = slot // SLOTS

        @pl.when((phase == 0) & (c < chunks - 1))
        def _():
            prepare(c + 1)

        @pl.when((c < chunks - 1))
        def _():
            first = jnp.where(phase == 0, 0, jnp.where(phase == 1, 1, (blocks + 1) // 2))
            count = jnp.where(phase == 0, 1, jnp.where(phase == 1, (blocks + 1) // 2 - 1, blocks - (blocks + 1) // 2))

            @pl.loop(0, count)
            def _(i):
                block = (c + 1) * blocks + first + i - 1
                make_dz(block // blocks, lax.rem(block, blocks))
                targets(first + i)

        @pl.when(slot == last)
        def _():
            make_dz(chunks - 1, blocks - 1)

        @pl.when((phase == 0) & (c < chunks))
        def _():
            make_dx(c)

        k = slot - last - 1
        block = k - (k + 2) // 4

        @pl.when((k >= 0) & (lax.rem(k + 3, 4) != 0) & (block < de_blocks))
        def _():
            make_de(block)

    for d in range(1, n_tp):
        everyone(fin_buf, fin_send, fin_recv, d).wait_recv()
    fin = functools.reduce(jnp.add, [fin_buf[k] for k in range(n_tp)])
    lanes = width // LANES
    loss = jnp.sum(slz_acc[:, 0:1], axis=0, keepdims=True) - jnp.sum(fin[lanes:lanes + 1, :], axis=1, keepdims=True)
    fin_ref[...] = fin
    fin_ref[pl.ds(lanes, 1), :] = jnp.broadcast_to(loss, (1, LANES))

    for d in range(1, n_tp):
        everyone(stat_buf, stat_send, stat_recv, d).wait_send()
        everyone(fin_buf, fin_send, fin_recv, d).wait_send()

    @pl.loop(0, chunks)
    def _(c):
        for kind in range(KINDS):
            rdma(c, kind).wait_send()
        put_dh(c).wait()

    for k in (de_blocks - 2, de_blocks - 1):
        put_de(k).wait()


def solution(mesh):
    n_tp = mesh.shape['tp']

    def local_step(hidden, norm_gain, emb_block, teacher_ids, teacher_q):
        tokens, width = hidden.shape
        vocab = emb_block.shape[0]
        count = teacher_ids.shape[1]
        chunks = tokens // CHUNK
        half = CHUNK // 2
        bit = half // (n_tp // 2) // 2
        f32, bf16 = jnp.float32, jnp.bfloat16
        dma = pltpu.SemaphoreType.DMA
        hbm, vmem = pl.BlockSpec(memory_space=pl.ANY), pl.BlockSpec(memory_space=pltpu.VMEM)
        dh, grad_block, fin = pl.pallas_call(
            functools.partial(kernel, n_tp),
            out_shape=(jax.ShapeDtypeStruct((tokens, width), bf16), jax.ShapeDtypeStruct((vocab, width), f32), jax.ShapeDtypeStruct((16, LANES), f32)),
            in_specs=[hbm, vmem, hbm, hbm, hbm],
            out_specs=(hbm, hbm, vmem),
            scratch_shapes=[
                pltpu.VMEM((tokens, width), bf16), pltpu.VMEM((vocab, width), bf16), pltpu.VMEM((tokens, count), jnp.int32), pltpu.VMEM((tokens, count), f32),
                pltpu.VMEM((tokens, width), bf16), pltpu.VMEM((vocab // BLOCK, tokens, BLOCK), f32), pltpu.VMEM((tokens, vocab), bf16), pltpu.VMEM((tokens, LANES), f32),
                *[pltpu.VMEM((CHUNK, count), f32)] * 5, pltpu.VMEM((CHUNK * (vocab // LANES + 1), LANES), f32),
                pltpu.VMEM((chunks, CHUNK, width), f32), pltpu.VMEM((chunks, half, width), f32), pltpu.VMEM((chunks, 6, bit, width), f32),
                pltpu.VMEM((chunks, CHUNK, width), f32), pltpu.VMEM((tokens, width), bf16), pltpu.VMEM((2, BLOCK, width), f32),
                pltpu.VMEM((8, width), f32), pltpu.VMEM((8, LANES), f32), pltpu.VMEM((8, LANES), f32),
                pltpu.VMEM((n_tp, 2 * tokens // LANES, LANES), f32), pltpu.VMEM((n_tp, 16, LANES), f32),
                dma((3,)), dma((vocab // BLOCK,)), dma((vocab // BLOCK,)), dma((chunks,)),
                dma((n_tp - 1,)), dma((n_tp - 1,)), dma((n_tp - 1,)), dma((n_tp - 1,)), dma((chunks, KINDS)), dma((chunks, KINDS)),
            ],
            compiler_params=pltpu.CompilerParams(collective_id=0, has_side_effects=True, vmem_limit_bytes=60 * 2**20),
        )(hidden, norm_gain, emb_block, teacher_ids, teacher_q)
        lanes = width // LANES
        return fin[lanes, :1], dh, fin[:lanes].reshape(-1), grad_block

    return jax.shard_map(local_step, mesh=mesh, in_specs=(P('dp', None), P(None), P('tp', None), P('dp', None), P('dp', None)), out_specs=(P('dp'), P('dp', None), P('dp'), P(('dp', 'tp'), None)), check_vma=False)
```

```python
import functools

import jax
import jax.numpy as jnp
from jax import lax
from jax.experimental import pallas as pl
from jax.experimental.pallas import tpu as pltpu
from jax.sharding import PartitionSpec as P

LANES = 128
CHUNK = 128
BLOCK = 256
SUB = 32
MESH = pl.DeviceIdType.MESH
SLOTS = 3
LAG_A, LAG_B, LAG_C, LAG_D, LAG_E, LAG_F = 2, 6, 10, 14, 17, 18
(K_SIB, K_FAR_R, K_FAR_L, K_NEAR_R, K_NEAR_L, K_SUM_R, K_SUM_L, K_OUT_R, K_OUT_L, K_OUT_S,
 K_PASS_R, K_PASS_L, K_FWD_L, K_FWD_R, K_FWD_O) = range(15)
KINDS = 15


def build_targets(lo_ref, code_ref, dense_ref, first, tokens, groups):
    count = lo_ref.shape[1]
    sub, half = 16, LANES // 2
    base = lax.broadcasted_iota(jnp.int32, (sub, count), 0).astype(jnp.float32).astype(jnp.bfloat16)
    slot = (lax.broadcasted_iota(jnp.int32, (sub, count), 1) + 1).astype(jnp.float32).astype(jnp.bfloat16)
    zero = jnp.zeros((sub, count), jnp.bfloat16)
    one = jnp.ones((sub, count), jnp.bfloat16)

    def row(ref, n):
        return jnp.broadcast_to(ref[pl.ds(n, 1), :], (sub, count)).astype(jnp.bfloat16)

    def one_token(n):
        lo, code = row(lo_ref, n), row(code_ref, n)
        low_hot = jnp.concatenate([jnp.where(lo == base + jnp.bfloat16(sub * k), one, zero) for k in range(half // sub)], axis=0)
        lhs = jnp.concatenate([jnp.where(code == base + jnp.bfloat16(sub * k), slot, zero) for k in range(2 * groups // sub)], axis=0)
        out = lax.dot_general(lhs, low_hot, (((1,), (1,)), ((), ())), preferred_element_type=jnp.float32)
        dense_ref[pl.ds(n * (groups + 1), groups), :] = jnp.concatenate([out[:groups], out[groups:]], axis=1)

    for u in range(tokens):
        one_token(first + u)


def take(table, lane):
    dims = lax.GatherDimensionNumbers(offset_dims=(), collapsed_slice_dims=(1,), start_index_map=(1,), operand_batching_dims=(0,), start_indices_batching_dims=(0,))
    return lax.gather(table, lane[..., None], dims, slice_sizes=(1, 1), mode=lax.GatherScatterMode.PROMISE_IN_BOUNDS)


def kernel(n_tp, hid_hbm, gain_ref, emb_hbm, ids_hbm, q_hbm, dh_hbm, x_hbm, dz_hbm, fin_ref,
           hid, emb, ids, q, xs, z, dz, lz_s, lo_s, code_s, dense, part, sib_buf, ring_buf,
           grad, dh_s, dw_acc, loss_acc, slz_acc, stat_buf, fin_buf,
           in_sem, emb_sem, out_sem, dh_sem, x_sem, stat_send, stat_recv, fin_send, fin_recv, send_sem, recv_sem):
    tokens, width = hid.shape
    vocab = emb.shape[0]
    groups = vocab // LANES
    chunks = tokens // CHUNK
    chips = n_tp // 2
    half = CHUNK // 2
    own = half // chips
    bit = own // 2
    scale = 1.0 / tokens
    dp, me = lax.axis_index('dp'), lax.axis_index('tp')
    core = lax.rem(me, 2)
    chip = me // 2
    right = lax.rem(chip + 1, chips)
    left = lax.rem(chip + chips - 1, chips)
    far = lax.rem(chip + 2, chips)
    to_right, to_left, to_sib = right * 2 + core, left * 2 + core, chip * 2 + 1 - core

    barrier = pltpu.get_barrier_semaphore()
    for d in range(1, n_tp):
        pl.semaphore_signal(barrier, inc=1, device_id=(dp, lax.rem(me + d, n_tp)), device_id_type=MESH)

    get_hid = pltpu.make_async_copy(hid_hbm, hid, in_sem.at[0])
    get_ids = pltpu.make_async_copy(ids_hbm, ids, in_sem.at[1])
    get_q = pltpu.make_async_copy(q_hbm, q, in_sem.at[2])

    def get_emb(b):
        rows = pl.ds(pl.multiple_of(b * BLOCK, BLOCK), BLOCK)
        return pltpu.make_async_copy(emb_hbm.at[rows], emb.at[rows], emb_sem.at[b])

    get_hid.start()
    for b in range(vocab // BLOCK):
        get_emb(b).start()
    get_ids.start()
    get_q.start()

    get_hid.wait()
    gain = 1.0 + gain_ref[...].reshape(1, width)

    @pl.loop(0, tokens // 32)
    def _(i):
        rows = pl.ds(pl.multiple_of(i * 32, 32), 32)
        h = hid[rows, :].astype(jnp.float32)
        inv = lax.rsqrt(jnp.mean(h * h, axis=1, keepdims=True) + 1e-6)
        xs[rows, :] = (h * inv * gain).astype(jnp.bfloat16)

    @pl.loop(0, vocab // BLOCK)
    def _(b):
        get_emb(b).wait()
        rows = pl.ds(pl.multiple_of(b * BLOCK, BLOCK), BLOCK)
        m = min(512, tokens)
        for r in range(0, tokens, m):
            z[b, pl.ds(r, m), :] = lax.dot_general(xs[pl.ds(r, m), :], emb[rows, :], (((1,), (1,)), ((), ())), preferred_element_type=jnp.float32)

    eye = lax.broadcasted_iota(jnp.int32, (LANES, LANES), 0) == lax.broadcasted_iota(jnp.int32, (LANES, LANES), 1)

    def as_row(tile):
        return jnp.sum(jnp.where(eye, tile, 0.0), axis=0, keepdims=True)

    stat_rows = tokens // LANES

    @pl.loop(0, stat_rows)
    def _(t):
        for u in range(0, LANES, 32):
            rows = pl.ds(pl.multiple_of(t * LANES + u, 32), 32)
            tiles = [z[g // 2, rows, pl.ds((g % 2) * LANES, LANES)] for g in range(groups)]
            peak = functools.reduce(jnp.maximum, tiles)
            peak = jnp.broadcast_to(jnp.max(peak, axis=1, keepdims=True), (32, LANES))
            total = functools.reduce(jnp.add, [jnp.exp(v - peak) for v in tiles])
            lz_s[rows, :] = peak
            dense[pl.ds(u, 32), :] = jnp.broadcast_to(jnp.sum(total, axis=1, keepdims=True), (32, LANES))
        stat_buf[me, pl.ds(t, 1), :] = as_row(lz_s[pl.ds(pl.multiple_of(t * LANES, LANES), LANES), :])
        stat_buf[me, pl.ds(stat_rows + t, 1), :] = as_row(dense[pl.ds(0, LANES), :])

    def everyone(buf, send, recv, d):
        return pltpu.make_async_remote_copy(
            src_ref=buf.at[me], dst_ref=buf.at[me], send_sem=send.at[d - 1], recv_sem=recv.at[d - 1],
            device_id=(dp, lax.rem(me + d, n_tp)), device_id_type=MESH)

    pl.semaphore_wait(barrier, n_tp - 1)
    for d in range(1, n_tp):
        everyone(stat_buf, stat_send, stat_recv, d).start()

    get_ids.wait()
    get_q.wait()
    start = me * vocab

    def prepare(c):
        @pl.loop(0, CHUNK // 32)
        def _(i):
            rows = pl.ds(pl.multiple_of(i * 32, 32), 32)
            src = pl.ds(pl.multiple_of(c * CHUNK + i * 32, 32), 32)
            lid = ids[src, :] - start
            lo_s[rows, :] = jnp.bitwise_and(lid, LANES // 2 - 1).astype(jnp.float32)
            code = jnp.right_shift(lid, 7) + groups * jnp.bitwise_and(jnp.right_shift(lid, 6), 1)
            code_s[rows, :] = jnp.where((lid >= 0) & (lid < vocab), code, -1).astype(jnp.float32)

    blocks = CHUNK // SUB

    def targets(i):
        build_targets(lo_s, code_s, dense, i * SUB, SUB, groups)

    prepare(0)

    @pl.loop(0, blocks)
    def _(i):
        targets(i)

    for d in range(1, n_tp):
        everyone(stat_buf, stat_send, stat_recv, d).wait_recv()
    peaks = [stat_buf[k, pl.ds(0, stat_rows), :] for k in range(n_tp)]
    peak = functools.reduce(jnp.maximum, peaks)
    total = functools.reduce(jnp.add, [stat_buf[k, pl.ds(stat_rows, stat_rows), :] * jnp.exp(peaks[k] - peak) for k in range(n_tp)])
    log_z = peak + jnp.log(total)
    for t in range(stat_rows):
        tile = jnp.where(eye, jnp.broadcast_to(log_z[t:t + 1, :], (LANES, LANES)), 0.0)
        lz_s[pl.ds(t * LANES, LANES), :] = jnp.broadcast_to(jnp.sum(tile, axis=1, keepdims=True), (LANES, LANES))

    fin_buf[me] = jnp.zeros(fin_buf.shape[1:], jnp.float32)
    dw_acc[...] = jnp.zeros_like(dw_acc)
    loss_acc[...] = jnp.zeros_like(loss_acc)
    slz_acc[...] = jnp.zeros_like(slz_acc)

    mine = core * half
    theirs = half - mine

    def at(base, block, off=0):
        return base + block * own + off

    def rdma(c, kind):
        def rows(first, count):
            return pl.ds(pl.multiple_of(first, 8), count)

        if kind == K_SIB:
            src, dst, peer = part.at[c, rows(theirs, half)], sib_buf.at[c], to_sib
        elif kind in (K_FAR_R, K_FAR_L, K_NEAR_R, K_NEAR_L, K_SUM_R, K_SUM_L):
            first = {K_FAR_R: at(mine, far), K_FAR_L: at(mine, far, bit), K_NEAR_R: at(mine, right, bit),
                     K_NEAR_L: at(mine, left), K_SUM_R: at(mine, right), K_SUM_L: at(mine, left, bit)}[kind]
            src, dst = part.at[c, rows(first, bit)], ring_buf.at[c, kind - K_FAR_R]
            peer = to_right if kind in (K_FAR_R, K_NEAR_R, K_SUM_R) else to_left
        else:
            first, count, peer = {
                K_OUT_R: (at(mine, chip), own, to_right), K_OUT_L: (at(mine, chip), own, to_left), K_OUT_S: (at(mine, chip), own, to_sib),
                K_PASS_R: (at(mine, left), bit, to_right), K_PASS_L: (at(mine, right, bit), bit, to_left),
                K_FWD_L: (at(mine, left), own, to_sib), K_FWD_R: (at(mine, right), own, to_sib), K_FWD_O: (at(mine, far), own, to_sib)}[kind]
            src = dst = grad.at[c, rows(first, count)]
        return pltpu.make_async_remote_copy(src_ref=src, dst_ref=dst, send_sem=send_sem.at[c, kind], recv_sem=recv_sem.at[c, kind],
                                            device_id=(dp, peer), device_id_type=MESH)

    put_x = pltpu.make_async_copy(xs, x_hbm, x_sem)
    put_x.start()

    def put_dz(c):
        rows = pl.ds(pl.multiple_of(c * CHUNK, CHUNK), CHUNK)
        return pltpu.make_async_copy(dz.at[rows], dz_hbm.at[rows], out_sem.at[c])

    def put_dh(c):
        rows = pl.ds(pl.multiple_of(c * CHUNK, CHUNK), CHUNK)
        return pltpu.make_async_copy(dh_s.at[rows], dh_hbm.at[rows], dh_sem.at[c])

    def make_dz(c, i):
        r = pl.multiple_of(i * SUB, SUB)
        rows = pl.ds(pl.multiple_of(c * CHUNK + r, SUB), SUB)
        lz = lz_s[rows, :]
        q_lo, q_hi = q[rows, :LANES] * scale, q[rows, LANES:] * scale
        s = jnp.broadcast_to(jnp.sum(q_lo + q_hi, axis=1, keepdims=True), (SUB, LANES))
        acc = jnp.zeros((8, LANES), jnp.float32)
        for g in range(groups):
            v = z[g // 2, rows, pl.ds((g % 2) * LANES, LANES)]
            slot = dense[pl.ds(r * (groups + 1) + g, SUB, stride=groups + 1), :]
            lane = slot.astype(jnp.int32) - 1
            low = jnp.bitwise_and(lane, LANES - 1)
            target = jnp.where(slot < 0.5, 0.0, jnp.where(lane < LANES, take(q_lo, low), take(q_hi, low)))
            dz[rows, pl.ds(g * LANES, LANES)] = (jnp.exp(v - lz) * s - target).astype(jnp.bfloat16)
            acc += jnp.sum((target * v).reshape(SUB // 8, 8, LANES), axis=0)
        loss_acc[...] += acc
        slz_acc[...] += jnp.sum((s * lz).reshape(SUB // 8, 8, LANES), axis=0)

    def make_dx(c):
        part[c] = jnp.dot(dz[pl.ds(pl.multiple_of(c * CHUNK, CHUNK), CHUNK), :], emb[...], preferred_element_type=jnp.float32)
        rdma(c, K_SIB).start()
        put_dz(c).start()

    def part_rows(first, count):
        return pl.ds(pl.multiple_of(first, 8), count)

    def stage_a(c):
        rdma(c, K_SIB).wait_recv()
        rows = part_rows(mine, half)
        part[c, rows, :] += sib_buf[c]
        for kind in (K_FAR_R, K_FAR_L, K_NEAR_R, K_NEAR_L):
            rdma(c, kind).start()

    def stage_b(c):
        rdma(c, K_FAR_R).wait_recv()
        part[c, part_rows(at(mine, right), bit), :] += ring_buf[c, 0]
        rdma(c, K_SUM_R).start()
        rdma(c, K_FAR_L).wait_recv()
        part[c, part_rows(at(mine, left, bit), bit), :] += ring_buf[c, 1]
        rdma(c, K_SUM_L).start()

    def stage_c(c):
        for kind in (K_NEAR_R, K_NEAR_L, K_SUM_R, K_SUM_L):
            rdma(c, kind).wait_recv()
        dx = part[c, part_rows(at(mine, chip), own), :] + jnp.concatenate(
            [ring_buf[c, K_SUM_R - 1] + ring_buf[c, K_NEAR_L - 1], ring_buf[c, K_SUM_L - 1] + ring_buf[c, K_NEAR_R - 1]], axis=0)
        h = hid[pl.ds(pl.multiple_of(c * CHUNK + at(mine, chip), own), own), :].astype(jnp.float32)
        inv = lax.rsqrt(jnp.mean(h * h, axis=1, keepdims=True) + 1e-6)
        unit = h * inv
        dy = dx * gain
        grad[c, part_rows(at(mine, chip), own), :] = inv * (dy - unit * jnp.mean(dy * unit, axis=1, keepdims=True))
        dw_acc[...] += jnp.sum((dx * unit).reshape(own // 8, 8, width), axis=0)
        for kind in (K_OUT_R, K_OUT_L, K_OUT_S):
            rdma(c, kind).start()

        @pl.when(c == chunks - 1)
        def _():
            dw = jnp.sum(dw_acc[...], axis=0, keepdims=True)
            for i in range(width // LANES):
                fin_buf[me, pl.ds(i, 1), :] = dw[:, i * LANES:(i + 1) * LANES]
            fin_buf[me, pl.ds(width // LANES, 1), :] = jnp.sum(loss_acc[...], axis=0, keepdims=True)
            for d in range(1, n_tp):
                everyone(fin_buf, fin_send, fin_recv, d).start()

    def stage_d(c):
        rdma(c, K_OUT_R).wait_recv()
        rdma(c, K_PASS_R).start()
        rdma(c, K_FWD_L).start()
        rdma(c, K_OUT_L).wait_recv()
        rdma(c, K_PASS_L).start()
        rdma(c, K_FWD_R).start()

    def stage_e(c):
        rdma(c, K_PASS_R).wait_recv()
        rdma(c, K_PASS_L).wait_recv()
        rdma(c, K_FWD_O).start()

    def stage_f(c):
        for kind in (K_OUT_S, K_FWD_L, K_FWD_R, K_FWD_O):
            rdma(c, kind).wait_recv()
        dh_s[pl.ds(pl.multiple_of(c * CHUNK, CHUNK), CHUNK), :] = grad[c].astype(jnp.bfloat16)
        put_dh(c).start()

    stages = ((LAG_F, stage_f), (LAG_E, stage_e), (LAG_D, stage_d), (LAG_C, stage_c), (LAG_B, stage_b), (LAG_A, stage_a))

    @pl.loop(0, blocks - 1)
    def _(i):
        make_dz(0, i)

    last = SLOTS * (chunks - 1)

    @pl.loop(0, SLOTS * chunks + LAG_F - SLOTS + 1)
    def _(slot):
        for lag, stage in stages:
            since = slot - lag

            @pl.when((since >= 0) & (lax.rem(since + SLOTS * LAG_F, SLOTS) == 0) & (since < SLOTS * chunks))
            def _(since=since, stage=stage):
                stage(since // SLOTS)

        phase = lax.rem(slot, SLOTS)
        c = slot // SLOTS

        @pl.when((phase == 0) & (c < chunks - 1))
        def _():
            prepare(c + 1)

        @pl.when((c < chunks - 1))
        def _():
            first = jnp.where(phase == 0, 0, jnp.where(phase == 1, 1, (blocks + 1) // 2))
            count = jnp.where(phase == 0, 1, jnp.where(phase == 1, (blocks + 1) // 2 - 1, blocks - (blocks + 1) // 2))

            @pl.loop(0, count)
            def _(i):
                block = (c + 1) * blocks + first + i - 1
                make_dz(block // blocks, lax.rem(block, blocks))
                targets(first + i)

        @pl.when(slot == last)
        def _():
            make_dz(chunks - 1, blocks - 1)

        @pl.when((phase == 0) & (c < chunks))
        def _():
            make_dx(c)

    for d in range(1, n_tp):
        everyone(fin_buf, fin_send, fin_recv, d).wait_recv()
    fin = functools.reduce(jnp.add, [fin_buf[k] for k in range(n_tp)])
    lanes = width // LANES
    loss = jnp.sum(slz_acc[:, 0:1], axis=0, keepdims=True) - jnp.sum(fin[lanes:lanes + 1, :], axis=1, keepdims=True)
    fin_ref[...] = fin
    fin_ref[pl.ds(lanes, 1), :] = jnp.broadcast_to(loss, (1, LANES))

    for d in range(1, n_tp):
        everyone(stat_buf, stat_send, stat_recv, d).wait_send()
        everyone(fin_buf, fin_send, fin_recv, d).wait_send()

    @pl.loop(0, chunks)
    def _(c):
        for kind in range(KINDS):
            rdma(c, kind).wait_send()
        put_dh(c).wait()
        put_dz(c).wait()

    put_x.wait()


def solution(mesh):
    n_tp = mesh.shape['tp']

    def local_step(hidden, norm_gain, emb_block, teacher_ids, teacher_q):
        tokens, width = hidden.shape
        vocab = emb_block.shape[0]
        count = teacher_ids.shape[1]
        chunks = tokens // CHUNK
        half = CHUNK // 2
        bit = half // (n_tp // 2) // 2
        f32, bf16 = jnp.float32, jnp.bfloat16
        dma = pltpu.SemaphoreType.DMA
        hbm, vmem = pl.BlockSpec(memory_space=pl.ANY), pl.BlockSpec(memory_space=pltpu.VMEM)
        dh, x_in, grad_z, fin = pl.pallas_call(
            functools.partial(kernel, n_tp),
            out_shape=(jax.ShapeDtypeStruct((tokens, width), bf16), jax.ShapeDtypeStruct((tokens, width), bf16),
                       jax.ShapeDtypeStruct((tokens, vocab), bf16), jax.ShapeDtypeStruct((16, LANES), f32)),
            in_specs=[hbm, vmem, hbm, hbm, hbm],
            out_specs=(hbm, hbm, hbm, vmem),
            scratch_shapes=[
                pltpu.VMEM((tokens, width), bf16), pltpu.VMEM((vocab, width), bf16), pltpu.VMEM((tokens, count), jnp.int32), pltpu.VMEM((tokens, count), f32),
                pltpu.VMEM((tokens, width), bf16), pltpu.VMEM((vocab // BLOCK, tokens, BLOCK), f32), pltpu.VMEM((tokens, vocab), bf16), pltpu.VMEM((tokens, LANES), f32),
                *[pltpu.VMEM((CHUNK, count), f32)] * 2, pltpu.VMEM((CHUNK * (vocab // LANES + 1), LANES), f32),
                pltpu.VMEM((chunks, CHUNK, width), f32), pltpu.VMEM((chunks, half, width), f32), pltpu.VMEM((chunks, 6, bit, width), f32),
                pltpu.VMEM((chunks, CHUNK, width), f32), pltpu.VMEM((tokens, width), bf16),
                pltpu.VMEM((8, width), f32), pltpu.VMEM((8, LANES), f32), pltpu.VMEM((8, LANES), f32),
                pltpu.VMEM((n_tp, 2 * tokens // LANES, LANES), f32), pltpu.VMEM((n_tp, 16, LANES), f32),
                dma((3,)), dma((vocab // BLOCK,)), dma((chunks,)), dma((chunks,)), dma(()),
                dma((n_tp - 1,)), dma((n_tp - 1,)), dma((n_tp - 1,)), dma((n_tp - 1,)), dma((chunks, KINDS)), dma((chunks, KINDS)),
            ],
            compiler_params=pltpu.CompilerParams(collective_id=0, has_side_effects=True, vmem_limit_bytes=60 * 2**20),
        )(hidden, norm_gain, emb_block, teacher_ids, teacher_q)
        grad_block = lax.dot_general(grad_z, x_in, (((0,), (0,)), ((), ())), preferred_element_type=f32)
        lanes = width // LANES
        return fin[lanes, :1], dh, fin[:lanes].reshape(-1), grad_block

    return jax.shard_map(local_step, mesh=mesh, in_specs=(P('dp', None), P(None), P('tp', None), P('dp', None), P('dp', None)), out_specs=(P('dp'), P('dp', None), P('dp'), P(('dp', 'tp'), None)), check_vma=False)
```

```python
import functools

import jax
import jax.numpy as jnp
from jax import lax
from jax.experimental import pallas as pl
from jax.experimental.pallas import tpu as pltpu
from jax.sharding import PartitionSpec as P

LANES = 128
CHUNK = 128
BLOCK = 256
SUB = 32
MESH = pl.DeviceIdType.MESH
SLOTS = 3
LAG_A, LAG_B, LAG_C, LAG_D, LAG_E, LAG_F = 2, 6, 10, 14, 17, 18
(K_SIB, K_FAR_R, K_FAR_L, K_NEAR_R, K_NEAR_L, K_SUM_R, K_SUM_L, K_OUT_R, K_OUT_L, K_OUT_S,
 K_PASS_R, K_PASS_L, K_FWD_L, K_FWD_R, K_FWD_O) = range(15)
KINDS = 15


def build_targets(lo_ref, code_ref, dense_ref, first, tokens, groups):
    count = lo_ref.shape[1]
    sub, half = 16, LANES // 2
    base = lax.broadcasted_iota(jnp.int32, (sub, count), 0).astype(jnp.float32).astype(jnp.bfloat16)
    slot = (lax.broadcasted_iota(jnp.int32, (sub, count), 1) + 1).astype(jnp.float32).astype(jnp.bfloat16)
    zero = jnp.zeros((sub, count), jnp.bfloat16)
    one = jnp.ones((sub, count), jnp.bfloat16)

    def row(ref, n):
        return jnp.broadcast_to(ref[pl.ds(n, 1), :], (sub, count)).astype(jnp.bfloat16)

    def one_token(n):
        lo, code = row(lo_ref, n), row(code_ref, n)
        low_hot = jnp.concatenate([jnp.where(lo == base + jnp.bfloat16(sub * k), one, zero) for k in range(half // sub)], axis=0)
        lhs = jnp.concatenate([jnp.where(code == base + jnp.bfloat16(sub * k), slot, zero) for k in range(2 * groups // sub)], axis=0)
        out = lax.dot_general(lhs, low_hot, (((1,), (1,)), ((), ())), preferred_element_type=jnp.float32)
        dense_ref[pl.ds(n * (groups + 1), groups), :] = jnp.concatenate([out[:groups], out[groups:]], axis=1)

    for u in range(tokens):
        one_token(first + u)


def take(table, lane):
    dims = lax.GatherDimensionNumbers(offset_dims=(), collapsed_slice_dims=(1,), start_index_map=(1,), operand_batching_dims=(0,), start_indices_batching_dims=(0,))
    return lax.gather(table, lane[..., None], dims, slice_sizes=(1, 1), mode=lax.GatherScatterMode.PROMISE_IN_BOUNDS)


def kernel(n_tp, hid_hbm, gain_ref, emb_hbm, ids_hbm, q_hbm, dh_hbm, x_hbm, dz_hbm, fin_ref,
           hid, emb, ids, q, xs, z, dz, lz_s, peak_s, sum_s, lo_s, code_s, dense, part, sib_buf, ring_buf,
           grad, dh_s, dw_acc, loss_acc, slz_acc, stat_buf, fin_buf,
           in_sem, emb_sem, out_sem, dh_sem, x_sem, stat_send, stat_recv, fin_send, fin_recv, send_sem, recv_sem):
    tokens, width = hid.shape
    vocab = emb.shape[0]
    groups = vocab // LANES
    chunks = tokens // CHUNK
    chips = n_tp // 2
    half = CHUNK // 2
    own = half // chips
    bit = own // 2
    scale = 1.0 / tokens
    dp, me = lax.axis_index('dp'), lax.axis_index('tp')
    core = lax.rem(me, 2)
    chip = me // 2
    right = lax.rem(chip + 1, chips)
    left = lax.rem(chip + chips - 1, chips)
    far = lax.rem(chip + 2, chips)
    to_right, to_left, to_sib = right * 2 + core, left * 2 + core, chip * 2 + 1 - core

    barrier = pltpu.get_barrier_semaphore()
    for d in range(1, n_tp):
        pl.semaphore_signal(barrier, inc=1, device_id=(dp, lax.rem(me + d, n_tp)), device_id_type=MESH)

    get_hid = pltpu.make_async_copy(hid_hbm, hid, in_sem.at[0])
    get_ids = pltpu.make_async_copy(ids_hbm, ids, in_sem.at[1])
    get_q = pltpu.make_async_copy(q_hbm, q, in_sem.at[2])

    def get_emb(b):
        rows = pl.ds(pl.multiple_of(b * BLOCK, BLOCK), BLOCK)
        return pltpu.make_async_copy(emb_hbm.at[rows], emb.at[rows], emb_sem.at[b])

    get_hid.start()
    get_hid.wait()
    for b in range(vocab // BLOCK):
        get_emb(b).start()
    get_ids.start()
    get_q.start()

    gain = 1.0 + gain_ref[...].reshape(1, width)

    @pl.loop(0, tokens // 32)
    def _(i):
        rows = pl.ds(pl.multiple_of(i * 32, 32), 32)
        h = hid[rows, :].astype(jnp.float32)
        inv = lax.rsqrt(jnp.mean(h * h, axis=1, keepdims=True) + 1e-6)
        xs[rows, :] = (h * inv * gain).astype(jnp.bfloat16)

    peak_s[...] = jnp.full(peak_s.shape, -jnp.inf, jnp.float32)
    sum_s[...] = jnp.zeros(sum_s.shape, jnp.float32)

    def lane_stats(b, first, count):
        for r in range(0, count, 32):
            rows = pl.ds(first + r, 32)
            tiles = [z[b, rows, pl.ds(g * LANES, LANES)] for g in range(BLOCK // LANES)]
            old = peak_s[rows, :]
            new = functools.reduce(jnp.maximum, tiles, old)
            sum_s[rows, :] = functools.reduce(jnp.add, [jnp.exp(v - new) for v in tiles], sum_s[rows, :] * jnp.exp(old - new))
            peak_s[rows, :] = new

    m = min(512, tokens)

    def logits(b, r):
        rows = pl.ds(pl.multiple_of(b * BLOCK, BLOCK), BLOCK)
        z[b, pl.ds(r, m), :] = lax.dot_general(xs[pl.ds(r, m), :], emb[rows, :], (((1,), (1,)), ((), ())), preferred_element_type=jnp.float32)

    get_emb(0).wait()
    for r in range(0, tokens, m):
        logits(0, r)

    @pl.loop(1, vocab // BLOCK)
    def _(b):
        get_emb(b).wait()
        for r in range(0, tokens, m):
            lane_stats(b - 1, r, m)
            logits(b, r)

    eye = lax.broadcasted_iota(jnp.int32, (LANES, LANES), 0) == lax.broadcasted_iota(jnp.int32, (LANES, LANES), 1)

    def as_row(tile):
        return jnp.sum(jnp.where(eye, tile, 0.0), axis=0, keepdims=True)

    stat_rows = tokens // LANES

    @pl.loop(0, stat_rows)
    def _(t):
        first = pl.multiple_of(t * LANES, LANES)
        lane_stats(vocab // BLOCK - 1, first, LANES)
        rows = pl.ds(first, LANES)
        lane_peak = peak_s[rows, :]
        peak = jnp.broadcast_to(jnp.max(lane_peak, axis=1, keepdims=True), (LANES, LANES))
        total = jnp.sum(sum_s[rows, :] * jnp.exp(lane_peak - peak), axis=1, keepdims=True)
        stat_buf[me, pl.ds(t, 1), :] = as_row(peak)
        stat_buf[me, pl.ds(stat_rows + t, 1), :] = as_row(jnp.broadcast_to(total, (LANES, LANES)))

    def everyone(buf, send, recv, d):
        return pltpu.make_async_remote_copy(
            src_ref=buf.at[me], dst_ref=buf.at[me], send_sem=send.at[d - 1], recv_sem=recv.at[d - 1],
            device_id=(dp, lax.rem(me + d, n_tp)), device_id_type=MESH)

    pl.semaphore_wait(barrier, n_tp - 1)
    for d in range(1, n_tp):
        everyone(stat_buf, stat_send, stat_recv, d).start()

    get_ids.wait()
    get_q.wait()
    start = me * vocab

    def prepare(c):
        @pl.loop(0, CHUNK // 32)
        def _(i):
            rows = pl.ds(pl.multiple_of(i * 32, 32), 32)
            src = pl.ds(pl.multiple_of(c * CHUNK + i * 32, 32), 32)
            lid = ids[src, :] - start
            lo_s[rows, :] = jnp.bitwise_and(lid, LANES // 2 - 1).astype(jnp.float32)
            code = jnp.right_shift(lid, 7) + groups * jnp.bitwise_and(jnp.right_shift(lid, 6), 1)
            code_s[rows, :] = jnp.where((lid >= 0) & (lid < vocab), code, -1).astype(jnp.float32)

    blocks = CHUNK // SUB

    def targets(i):
        build_targets(lo_s, code_s, dense, i * SUB, SUB, groups)

    prepare(0)

    @pl.loop(0, blocks)
    def _(i):
        targets(i)

    for d in range(1, n_tp):
        everyone(stat_buf, stat_send, stat_recv, d).wait_recv()
    peaks = [stat_buf[k, pl.ds(0, stat_rows), :] for k in range(n_tp)]
    peak = functools.reduce(jnp.maximum, peaks)
    total = functools.reduce(jnp.add, [stat_buf[k, pl.ds(stat_rows, stat_rows), :] * jnp.exp(peaks[k] - peak) for k in range(n_tp)])
    log_z = peak + jnp.log(total)
    for t in range(stat_rows):
        tile = jnp.where(eye, jnp.broadcast_to(log_z[t:t + 1, :], (LANES, LANES)), 0.0)
        lz_s[pl.ds(t * LANES, LANES), :] = jnp.broadcast_to(jnp.sum(tile, axis=1, keepdims=True), (LANES, LANES))

    fin_buf[me] = jnp.zeros(fin_buf.shape[1:], jnp.float32)
    dw_acc[...] = jnp.zeros_like(dw_acc)
    loss_acc[...] = jnp.zeros_like(loss_acc)
    slz_acc[...] = jnp.zeros_like(slz_acc)

    mine = core * half
    theirs = half - mine

    def at(base, block, off=0):
        return base + block * own + off

    def rdma(c, kind):
        def rows(first, count):
            return pl.ds(pl.multiple_of(first, 8), count)

        if kind == K_SIB:
            src, dst, peer = part.at[c, rows(theirs, half)], sib_buf.at[c], to_sib
        elif kind in (K_FAR_R, K_FAR_L, K_NEAR_R, K_NEAR_L, K_SUM_R, K_SUM_L):
            first = {K_FAR_R: at(mine, far), K_FAR_L: at(mine, far, bit), K_NEAR_R: at(mine, right, bit),
                     K_NEAR_L: at(mine, left), K_SUM_R: at(mine, right), K_SUM_L: at(mine, left, bit)}[kind]
            src, dst = part.at[c, rows(first, bit)], ring_buf.at[c, kind - K_FAR_R]
            peer = to_right if kind in (K_FAR_R, K_NEAR_R, K_SUM_R) else to_left
        else:
            first, count, peer = {
                K_OUT_R: (at(mine, chip), own, to_right), K_OUT_L: (at(mine, chip), own, to_left), K_OUT_S: (at(mine, chip), own, to_sib),
                K_PASS_R: (at(mine, left), bit, to_right), K_PASS_L: (at(mine, right, bit), bit, to_left),
                K_FWD_L: (at(mine, left), own, to_sib), K_FWD_R: (at(mine, right), own, to_sib), K_FWD_O: (at(mine, far), own, to_sib)}[kind]
            src = dst = grad.at[c, rows(first, count)]
        return pltpu.make_async_remote_copy(src_ref=src, dst_ref=dst, send_sem=send_sem.at[c, kind], recv_sem=recv_sem.at[c, kind],
                                            device_id=(dp, peer), device_id_type=MESH)

    put_x = pltpu.make_async_copy(xs, x_hbm, x_sem)
    put_x.start()

    def put_dz(c):
        rows = pl.ds(pl.multiple_of(c * CHUNK, CHUNK), CHUNK)
        return pltpu.make_async_copy(dz.at[rows], dz_hbm.at[rows], out_sem.at[c])

    def put_dh(c):
        rows = pl.ds(pl.multiple_of(c * CHUNK, CHUNK), CHUNK)
        return pltpu.make_async_copy(dh_s.at[rows], dh_hbm.at[rows], dh_sem.at[c])

    def make_dz(c, i):
        r = pl.multiple_of(i * SUB, SUB)
        rows = pl.ds(pl.multiple_of(c * CHUNK + r, SUB), SUB)
        lz = lz_s[rows, :]
        q_lo, q_hi = q[rows, :LANES] * scale, q[rows, LANES:] * scale
        s = jnp.broadcast_to(jnp.sum(q_lo + q_hi, axis=1, keepdims=True), (SUB, LANES))
        acc = jnp.zeros((8, LANES), jnp.float32)
        for g in range(groups):
            v = z[g // 2, rows, pl.ds((g % 2) * LANES, LANES)]
            slot = dense[pl.ds(r * (groups + 1) + g, SUB, stride=groups + 1), :]
            lane = slot.astype(jnp.int32) - 1
            low = jnp.bitwise_and(lane, LANES - 1)
            target = jnp.where(slot < 0.5, 0.0, jnp.where(lane < LANES, take(q_lo, low), take(q_hi, low)))
            dz[rows, pl.ds(g * LANES, LANES)] = (jnp.exp(v - lz) * s - target).astype(jnp.bfloat16)
            acc += jnp.sum((target * v).reshape(SUB // 8, 8, LANES), axis=0)
        loss_acc[...] += acc
        slz_acc[...] += jnp.sum((s * lz).reshape(SUB // 8, 8, LANES), axis=0)

    def make_dx(c):
        part[c] = jnp.dot(dz[pl.ds(pl.multiple_of(c * CHUNK, CHUNK), CHUNK), :], emb[...], preferred_element_type=jnp.float32)
        rdma(c, K_SIB).start()
        put_dz(c).start()

    def part_rows(first, count):
        return pl.ds(pl.multiple_of(first, 8), count)

    def stage_a(c):
        rdma(c, K_SIB).wait_recv()
        rows = part_rows(mine, half)
        part[c, rows, :] += sib_buf[c]
        for kind in (K_FAR_R, K_FAR_L, K_NEAR_R, K_NEAR_L):
            rdma(c, kind).start()

    def stage_b(c):
        rdma(c, K_FAR_R).wait_recv()
        part[c, part_rows(at(mine, right), bit), :] += ring_buf[c, 0]
        rdma(c, K_SUM_R).start()
        rdma(c, K_FAR_L).wait_recv()
        part[c, part_rows(at(mine, left, bit), bit), :] += ring_buf[c, 1]
        rdma(c, K_SUM_L).start()

    def stage_c(c):
        for kind in (K_NEAR_R, K_NEAR_L, K_SUM_R, K_SUM_L):
            rdma(c, kind).wait_recv()
        dx = part[c, part_rows(at(mine, chip), own), :] + jnp.concatenate(
            [ring_buf[c, K_SUM_R - 1] + ring_buf[c, K_NEAR_L - 1], ring_buf[c, K_SUM_L - 1] + ring_buf[c, K_NEAR_R - 1]], axis=0)
        h = hid[pl.ds(pl.multiple_of(c * CHUNK + at(mine, chip), own), own), :].astype(jnp.float32)
        inv = lax.rsqrt(jnp.mean(h * h, axis=1, keepdims=True) + 1e-6)
        unit = h * inv
        dy = dx * gain
        grad[c, part_rows(at(mine, chip), own), :] = inv * (dy - unit * jnp.mean(dy * unit, axis=1, keepdims=True))
        dw_acc[...] += jnp.sum((dx * unit).reshape(own // 8, 8, width), axis=0)
        for kind in (K_OUT_R, K_OUT_L, K_OUT_S):
            rdma(c, kind).start()

        @pl.when(c == chunks - 1)
        def _():
            dw = jnp.sum(dw_acc[...], axis=0, keepdims=True)
            for i in range(width // LANES):
                fin_buf[me, pl.ds(i, 1), :] = dw[:, i * LANES:(i + 1) * LANES]
            fin_buf[me, pl.ds(width // LANES, 1), :] = jnp.sum(loss_acc[...], axis=0, keepdims=True)
            for d in range(1, n_tp):
                everyone(fin_buf, fin_send, fin_recv, d).start()

    def stage_d(c):
        rdma(c, K_OUT_R).wait_recv()
        rdma(c, K_PASS_R).start()
        rdma(c, K_FWD_L).start()
        rdma(c, K_OUT_L).wait_recv()
        rdma(c, K_PASS_L).start()
        rdma(c, K_FWD_R).start()

    def stage_e(c):
        rdma(c, K_PASS_R).wait_recv()
        rdma(c, K_PASS_L).wait_recv()
        rdma(c, K_FWD_O).start()

    def stage_f(c):
        for kind in (K_OUT_S, K_FWD_L, K_FWD_R, K_FWD_O):
            rdma(c, kind).wait_recv()
        dh_s[pl.ds(pl.multiple_of(c * CHUNK, CHUNK), CHUNK), :] = grad[c].astype(jnp.bfloat16)
        put_dh(c).start()

    stages = ((LAG_F, stage_f), (LAG_E, stage_e), (LAG_D, stage_d), (LAG_C, stage_c), (LAG_B, stage_b), (LAG_A, stage_a))

    @pl.loop(0, blocks - 1)
    def _(i):
        make_dz(0, i)

    last = SLOTS * (chunks - 1)

    @pl.loop(0, SLOTS * chunks + LAG_F - SLOTS + 1)
    def _(slot):
        for lag, stage in stages:
            since = slot - lag

            @pl.when((since >= 0) & (lax.rem(since + SLOTS * LAG_F, SLOTS) == 0) & (since < SLOTS * chunks))
            def _(since=since, stage=stage):
                stage(since // SLOTS)

        phase = lax.rem(slot, SLOTS)
        c = slot // SLOTS

        @pl.when((phase == 0) & (c < chunks - 1))
        def _():
            prepare(c + 1)

        @pl.when((c < chunks - 1))
        def _():
            first = jnp.where(phase == 0, 0, jnp.where(phase == 1, 1, (blocks + 1) // 2))
            count = jnp.where(phase == 0, 1, jnp.where(phase == 1, (blocks + 1) // 2 - 1, blocks - (blocks + 1) // 2))

            @pl.loop(0, count)
            def _(i):
                block = (c + 1) * blocks + first + i - 1
                make_dz(block // blocks, lax.rem(block, blocks))
                targets(first + i)

        @pl.when(slot == last)
        def _():
            make_dz(chunks - 1, blocks - 1)

        @pl.when((phase == 0) & (c < chunks))
        def _():
            make_dx(c)

    for d in range(1, n_tp):
        everyone(fin_buf, fin_send, fin_recv, d).wait_recv()
    fin = functools.reduce(jnp.add, [fin_buf[k] for k in range(n_tp)])
    lanes = width // LANES
    loss = jnp.sum(slz_acc[:, 0:1], axis=0, keepdims=True) - jnp.sum(fin[lanes:lanes + 1, :], axis=1, keepdims=True)
    fin_ref[...] = fin
    fin_ref[pl.ds(lanes, 1), :] = jnp.broadcast_to(loss, (1, LANES))

    for d in range(1, n_tp):
        everyone(stat_buf, stat_send, stat_recv, d).wait_send()
        everyone(fin_buf, fin_send, fin_recv, d).wait_send()

    @pl.loop(0, chunks)
    def _(c):
        for kind in range(KINDS):
            rdma(c, kind).wait_send()
        put_dh(c).wait()
        put_dz(c).wait()

    put_x.wait()


def solution(mesh):
    n_tp = mesh.shape['tp']

    def local_step(hidden, norm_gain, emb_block, teacher_ids, teacher_q):
        tokens, width = hidden.shape
        vocab = emb_block.shape[0]
        count = teacher_ids.shape[1]
        chunks = tokens // CHUNK
        half = CHUNK // 2
        bit = half // (n_tp // 2) // 2
        f32, bf16 = jnp.float32, jnp.bfloat16
        dma = pltpu.SemaphoreType.DMA
        hbm, vmem = pl.BlockSpec(memory_space=pl.ANY), pl.BlockSpec(memory_space=pltpu.VMEM)
        dh, x_in, grad_z, fin = pl.pallas_call(
            functools.partial(kernel, n_tp),
            out_shape=(jax.ShapeDtypeStruct((tokens, width), bf16), jax.ShapeDtypeStruct((tokens, width), bf16),
                       jax.ShapeDtypeStruct((tokens, vocab), bf16), jax.ShapeDtypeStruct((16, LANES), f32)),
            in_specs=[hbm, vmem, hbm, hbm, hbm],
            out_specs=(hbm, hbm, hbm, vmem),
            scratch_shapes=[
                pltpu.VMEM((tokens, width), bf16), pltpu.VMEM((vocab, width), bf16), pltpu.VMEM((tokens, count), jnp.int32), pltpu.VMEM((tokens, count), f32),
                pltpu.VMEM((tokens, width), bf16), pltpu.VMEM((vocab // BLOCK, tokens, BLOCK), f32), pltpu.VMEM((tokens, vocab), bf16), *[pltpu.VMEM((tokens, LANES), f32)] * 3,
                *[pltpu.VMEM((CHUNK, count), f32)] * 2, pltpu.VMEM((CHUNK * (vocab // LANES + 1), LANES), f32),
                pltpu.VMEM((chunks, CHUNK, width), f32), pltpu.VMEM((chunks, half, width), f32), pltpu.VMEM((chunks, 6, bit, width), f32),
                pltpu.VMEM((chunks, CHUNK, width), f32), pltpu.VMEM((tokens, width), bf16),
                pltpu.VMEM((8, width), f32), pltpu.VMEM((8, LANES), f32), pltpu.VMEM((8, LANES), f32),
                pltpu.VMEM((n_tp, 2 * tokens // LANES, LANES), f32), pltpu.VMEM((n_tp, 16, LANES), f32),
                dma((3,)), dma((vocab // BLOCK,)), dma((chunks,)), dma((chunks,)), dma(()),
                dma((n_tp - 1,)), dma((n_tp - 1,)), dma((n_tp - 1,)), dma((n_tp - 1,)), dma((chunks, KINDS)), dma((chunks, KINDS)),
            ],
            compiler_params=pltpu.CompilerParams(collective_id=0, has_side_effects=True, vmem_limit_bytes=60 * 2**20),
        )(hidden, norm_gain, emb_block, teacher_ids, teacher_q)
        grad_block = lax.dot_general(grad_z, x_in, (((0,), (0,)), ((), ())), preferred_element_type=f32)
        lanes = width // LANES
        return fin[lanes, :1], dh, fin[:lanes].reshape(-1), grad_block

    return jax.shard_map(local_step, mesh=mesh, in_specs=(P('dp', None), P(None), P('tp', None), P('dp', None), P('dp', None)), out_specs=(P('dp'), P('dp', None), P('dp'), P(('dp', 'tp'), None)), check_vma=False)
```

```python
import functools

import jax
import jax.numpy as jnp
from jax import lax
from jax.experimental import pallas as pl
from jax.experimental.pallas import tpu as pltpu
from jax.sharding import PartitionSpec as P

LANES = 128
CHUNK = 128
BLOCK = 256
SUB = 32
MESH = pl.DeviceIdType.MESH
SLOTS = 3
LAG_A, LAG_B, LAG_C, LAG_D, LAG_E, LAG_F = 2, 6, 10, 14, 17, 18
(K_SIB, K_FAR_R, K_FAR_L, K_NEAR_R, K_NEAR_L, K_SUM_R, K_SUM_L, K_OUT_R, K_OUT_L, K_OUT_S,
 K_PASS_R, K_PASS_L, K_FWD_L, K_FWD_R, K_FWD_O) = range(15)
KINDS = 15


def build_targets(lo_ref, code_ref, dense_ref, first, tokens, groups):
    count = lo_ref.shape[1]
    sub, half = 16, LANES // 2
    base = lax.broadcasted_iota(jnp.int32, (sub, count), 0).astype(jnp.float32).astype(jnp.bfloat16)
    slot = (lax.broadcasted_iota(jnp.int32, (sub, count), 1) + 1).astype(jnp.float32).astype(jnp.bfloat16)
    zero = jnp.zeros((sub, count), jnp.bfloat16)
    one = jnp.ones((sub, count), jnp.bfloat16)

    def row(ref, n):
        return jnp.broadcast_to(ref[pl.ds(n, 1), :], (sub, count)).astype(jnp.bfloat16)

    def one_token(n):
        lo, code = row(lo_ref, n), row(code_ref, n)
        low_hot = jnp.concatenate([jnp.where(lo == base + jnp.bfloat16(sub * k), one, zero) for k in range(half // sub)], axis=0)
        lhs = jnp.concatenate([jnp.where(code == base + jnp.bfloat16(sub * k), slot, zero) for k in range(2 * groups // sub)], axis=0)
        out = lax.dot_general(lhs, low_hot, (((1,), (1,)), ((), ())), preferred_element_type=jnp.float32)
        dense_ref[pl.ds(n * (groups + 1), groups), :] = jnp.concatenate([out[:groups], out[groups:]], axis=1)

    for u in range(tokens):
        one_token(first + u)


def take(table, lane):
    dims = lax.GatherDimensionNumbers(offset_dims=(), collapsed_slice_dims=(1,), start_index_map=(1,), operand_batching_dims=(0,), start_indices_batching_dims=(0,))
    return lax.gather(table, lane[..., None], dims, slice_sizes=(1, 1), mode=lax.GatherScatterMode.PROMISE_IN_BOUNDS)


def kernel(n_tp, hid_hbm, gain_ref, emb_hbm, ids_hbm, q_hbm, dh_hbm, x_hbm, dz_hbm, fin_ref,
           hid, emb, ids, q, xs, z, dz, lz_s, peak_s, sum_s, lo_s, code_s, dense, part, sib_buf, ring_buf,
           grad, dh_s, dw_acc, loss_acc, slz_acc, stat_buf, fin_buf,
           in_sem, emb_sem, out_sem, dh_sem, x_sem, stat_send, stat_recv, fin_send, fin_recv, send_sem, recv_sem):
    tokens, width = hid.shape
    vocab = emb.shape[0]
    groups = vocab // LANES
    chunks = tokens // CHUNK
    chips = n_tp // 2
    half = CHUNK // 2
    own = half // chips
    bit = own // 2
    scale = 1.0 / tokens
    dp, me = lax.axis_index('dp'), lax.axis_index('tp')
    core = lax.rem(me, 2)
    chip = me // 2
    right = lax.rem(chip + 1, chips)
    left = lax.rem(chip + chips - 1, chips)
    far = lax.rem(chip + 2, chips)
    to_right, to_left, to_sib = right * 2 + core, left * 2 + core, chip * 2 + 1 - core

    barrier = pltpu.get_barrier_semaphore()
    for d in range(1, n_tp):
        pl.semaphore_signal(barrier, inc=1, device_id=(dp, lax.rem(me + d, n_tp)), device_id_type=MESH)

    quarter = tokens // 4

    def get_hid(i):
        rows = pl.ds(pl.multiple_of(i * quarter, quarter), quarter)
        return pltpu.make_async_copy(hid_hbm.at[rows], hid.at[rows], in_sem.at[2 + i])

    get_ids = pltpu.make_async_copy(ids_hbm, ids, in_sem.at[0])
    get_q = pltpu.make_async_copy(q_hbm, q, in_sem.at[1])

    def get_emb(b):
        rows = pl.ds(pl.multiple_of(b * BLOCK, BLOCK), BLOCK)
        return pltpu.make_async_copy(emb_hbm.at[rows], emb.at[rows], emb_sem.at[b])

    for i in range(4):
        get_hid(i).start()
    for b in range(vocab // BLOCK):
        get_emb(b).start()
    get_ids.start()
    get_q.start()

    gain = 1.0 + gain_ref[...].reshape(1, width)

    @pl.loop(0, 4)
    def _(i):
        get_hid(i).wait()

        @pl.loop(0, quarter // 32)
        def _(j):
            rows = pl.ds(pl.multiple_of(i * quarter + j * 32, 32), 32)
            h = hid[rows, :].astype(jnp.float32)
            inv = lax.rsqrt(jnp.mean(h * h, axis=1, keepdims=True) + 1e-6)
            xs[rows, :] = (h * inv * gain).astype(jnp.bfloat16)

    peak_s[...] = jnp.full(peak_s.shape, -jnp.inf, jnp.float32)
    sum_s[...] = jnp.zeros(sum_s.shape, jnp.float32)

    def lane_stats(b, first, count):
        for r in range(0, count, 32):
            rows = pl.ds(first + r, 32)
            tiles = [z[b, rows, pl.ds(g * LANES, LANES)] for g in range(BLOCK // LANES)]
            old = peak_s[rows, :]
            new = functools.reduce(jnp.maximum, tiles, old)
            sum_s[rows, :] = functools.reduce(jnp.add, [jnp.exp(v - new) for v in tiles], sum_s[rows, :] * jnp.exp(old - new))
            peak_s[rows, :] = new

    m = min(512, tokens)

    def logits(b, r):
        rows = pl.ds(pl.multiple_of(b * BLOCK, BLOCK), BLOCK)
        z[b, pl.ds(r, m), :] = lax.dot_general(xs[pl.ds(r, m), :], emb[rows, :], (((1,), (1,)), ((), ())), preferred_element_type=jnp.float32)

    get_emb(0).wait()
    for r in range(0, tokens, m):
        logits(0, r)

    @pl.loop(1, vocab // BLOCK)
    def _(b):
        get_emb(b).wait()
        for r in range(0, tokens, m):
            lane_stats(b - 1, r, m)
            logits(b, r)

    eye = lax.broadcasted_iota(jnp.int32, (LANES, LANES), 0) == lax.broadcasted_iota(jnp.int32, (LANES, LANES), 1)

    def as_row(tile):
        return jnp.sum(jnp.where(eye, tile, 0.0), axis=0, keepdims=True)

    stat_rows = tokens // LANES

    @pl.loop(0, stat_rows)
    def _(t):
        first = pl.multiple_of(t * LANES, LANES)
        lane_stats(vocab // BLOCK - 1, first, LANES)
        rows = pl.ds(first, LANES)
        lane_peak = peak_s[rows, :]
        peak = jnp.broadcast_to(jnp.max(lane_peak, axis=1, keepdims=True), (LANES, LANES))
        total = jnp.sum(sum_s[rows, :] * jnp.exp(lane_peak - peak), axis=1, keepdims=True)
        stat_buf[me, pl.ds(t, 1), :] = as_row(peak)
        stat_buf[me, pl.ds(stat_rows + t, 1), :] = as_row(jnp.broadcast_to(total, (LANES, LANES)))

    def everyone(buf, send, recv, d):
        return pltpu.make_async_remote_copy(
            src_ref=buf.at[me], dst_ref=buf.at[me], send_sem=send.at[d - 1], recv_sem=recv.at[d - 1],
            device_id=(dp, lax.rem(me + d, n_tp)), device_id_type=MESH)

    pl.semaphore_wait(barrier, n_tp - 1)
    for d in range(1, n_tp):
        everyone(stat_buf, stat_send, stat_recv, d).start()

    get_ids.wait()
    get_q.wait()
    start = me * vocab

    def prepare(c):
        @pl.loop(0, CHUNK // 32)
        def _(i):
            rows = pl.ds(pl.multiple_of(i * 32, 32), 32)
            src = pl.ds(pl.multiple_of(c * CHUNK + i * 32, 32), 32)
            lid = ids[src, :] - start
            lo_s[rows, :] = jnp.bitwise_and(lid, LANES // 2 - 1).astype(jnp.float32)
            code = jnp.right_shift(lid, 7) + groups * jnp.bitwise_and(jnp.right_shift(lid, 6), 1)
            code_s[rows, :] = jnp.where((lid >= 0) & (lid < vocab), code, -1).astype(jnp.float32)

    blocks = CHUNK // SUB

    def targets(i):
        build_targets(lo_s, code_s, dense, i * SUB, SUB, groups)

    prepare(0)

    @pl.loop(0, blocks)
    def _(i):
        targets(i)

    for d in range(1, n_tp):
        everyone(stat_buf, stat_send, stat_recv, d).wait_recv()
    peaks = [stat_buf[k, pl.ds(0, stat_rows), :] for k in range(n_tp)]
    peak = functools.reduce(jnp.maximum, peaks)
    total = functools.reduce(jnp.add, [stat_buf[k, pl.ds(stat_rows, stat_rows), :] * jnp.exp(peaks[k] - peak) for k in range(n_tp)])
    log_z = peak + jnp.log(total)
    for t in range(stat_rows):
        tile = jnp.where(eye, jnp.broadcast_to(log_z[t:t + 1, :], (LANES, LANES)), 0.0)
        lz_s[pl.ds(t * LANES, LANES), :] = jnp.broadcast_to(jnp.sum(tile, axis=1, keepdims=True), (LANES, LANES))

    fin_buf[me] = jnp.zeros(fin_buf.shape[1:], jnp.float32)
    dw_acc[...] = jnp.zeros_like(dw_acc)
    loss_acc[...] = jnp.zeros_like(loss_acc)
    slz_acc[...] = jnp.zeros_like(slz_acc)

    mine = core * half
    theirs = half - mine

    def at(base, block, off=0):
        return base + block * own + off

    def rdma(c, kind):
        def rows(first, count):
            return pl.ds(pl.multiple_of(first, 8), count)

        if kind == K_SIB:
            src, dst, peer = part.at[c, rows(theirs, half)], sib_buf.at[c], to_sib
        elif kind in (K_FAR_R, K_FAR_L, K_NEAR_R, K_NEAR_L, K_SUM_R, K_SUM_L):
            first = {K_FAR_R: at(mine, far), K_FAR_L: at(mine, far, bit), K_NEAR_R: at(mine, right, bit),
                     K_NEAR_L: at(mine, left), K_SUM_R: at(mine, right), K_SUM_L: at(mine, left, bit)}[kind]
            src, dst = part.at[c, rows(first, bit)], ring_buf.at[c, kind - K_FAR_R]
            peer = to_right if kind in (K_FAR_R, K_NEAR_R, K_SUM_R) else to_left
        else:
            first, count, peer = {
                K_OUT_R: (at(mine, chip), own, to_right), K_OUT_L: (at(mine, chip), own, to_left), K_OUT_S: (at(mine, chip), own, to_sib),
                K_PASS_R: (at(mine, left), bit, to_right), K_PASS_L: (at(mine, right, bit), bit, to_left),
                K_FWD_L: (at(mine, left), own, to_sib), K_FWD_R: (at(mine, right), own, to_sib), K_FWD_O: (at(mine, far), own, to_sib)}[kind]
            src = dst = grad.at[c, rows(first, count)]
        return pltpu.make_async_remote_copy(src_ref=src, dst_ref=dst, send_sem=send_sem.at[c, kind], recv_sem=recv_sem.at[c, kind],
                                            device_id=(dp, peer), device_id_type=MESH)

    put_x = pltpu.make_async_copy(xs, x_hbm, x_sem)
    put_x.start()

    def put_dz(c):
        rows = pl.ds(pl.multiple_of(c * CHUNK, CHUNK), CHUNK)
        return pltpu.make_async_copy(dz.at[rows], dz_hbm.at[rows], out_sem.at[c])

    def put_dh(c):
        rows = pl.ds(pl.multiple_of(c * CHUNK, CHUNK), CHUNK)
        return pltpu.make_async_copy(dh_s.at[rows], dh_hbm.at[rows], dh_sem.at[c])

    def make_dz(c, i):
        r = pl.multiple_of(i * SUB, SUB)
        rows = pl.ds(pl.multiple_of(c * CHUNK + r, SUB), SUB)
        lz = lz_s[rows, :]
        q_lo, q_hi = q[rows, :LANES] * scale, q[rows, LANES:] * scale
        s = jnp.broadcast_to(jnp.sum(q_lo + q_hi, axis=1, keepdims=True), (SUB, LANES))
        acc = jnp.zeros((8, LANES), jnp.float32)
        for g in range(groups):
            v = z[g // 2, rows, pl.ds((g % 2) * LANES, LANES)]
            slot = dense[pl.ds(r * (groups + 1) + g, SUB, stride=groups + 1), :]
            lane = slot.astype(jnp.int32) - 1
            low = jnp.bitwise_and(lane, LANES - 1)
            target = jnp.where(slot < 0.5, 0.0, jnp.where(lane < LANES, take(q_lo, low), take(q_hi, low)))
            dz[rows, pl.ds(g * LANES, LANES)] = (jnp.exp(v - lz) * s - target).astype(jnp.bfloat16)
            acc += jnp.sum((target * v).reshape(SUB // 8, 8, LANES), axis=0)
        loss_acc[...] += acc
        slz_acc[...] += jnp.sum((s * lz).reshape(SUB // 8, 8, LANES), axis=0)

    def make_dx(c):
        part[c] = jnp.dot(dz[pl.ds(pl.multiple_of(c * CHUNK, CHUNK), CHUNK), :], emb[...], preferred_element_type=jnp.float32)
        rdma(c, K_SIB).start()
        put_dz(c).start()

    def part_rows(first, count):
        return pl.ds(pl.multiple_of(first, 8), count)

    def stage_a(c):
        rdma(c, K_SIB).wait_recv()
        rows = part_rows(mine, half)
        part[c, rows, :] += sib_buf[c]
        for kind in (K_FAR_R, K_FAR_L, K_NEAR_R, K_NEAR_L):
            rdma(c, kind).start()

    def stage_b(c):
        rdma(c, K_FAR_R).wait_recv()
        part[c, part_rows(at(mine, right), bit), :] += ring_buf[c, 0]
        rdma(c, K_SUM_R).start()
        rdma(c, K_FAR_L).wait_recv()
        part[c, part_rows(at(mine, left, bit), bit), :] += ring_buf[c, 1]
        rdma(c, K_SUM_L).start()

    def stage_c(c):
        for kind in (K_NEAR_R, K_NEAR_L, K_SUM_R, K_SUM_L):
            rdma(c, kind).wait_recv()
        dx = part[c, part_rows(at(mine, chip), own), :] + jnp.concatenate(
            [ring_buf[c, K_SUM_R - 1] + ring_buf[c, K_NEAR_L - 1], ring_buf[c, K_SUM_L - 1] + ring_buf[c, K_NEAR_R - 1]], axis=0)
        h = hid[pl.ds(pl.multiple_of(c * CHUNK + at(mine, chip), own), own), :].astype(jnp.float32)
        inv = lax.rsqrt(jnp.mean(h * h, axis=1, keepdims=True) + 1e-6)
        unit = h * inv
        dy = dx * gain
        grad[c, part_rows(at(mine, chip), own), :] = inv * (dy - unit * jnp.mean(dy * unit, axis=1, keepdims=True))
        dw_acc[...] += jnp.sum((dx * unit).reshape(own // 8, 8, width), axis=0)
        for kind in (K_OUT_R, K_OUT_L, K_OUT_S):
            rdma(c, kind).start()

        @pl.when(c == chunks - 1)
        def _():
            dw = jnp.sum(dw_acc[...], axis=0, keepdims=True)
            for i in range(width // LANES):
                fin_buf[me, pl.ds(i, 1), :] = dw[:, i * LANES:(i + 1) * LANES]
            fin_buf[me, pl.ds(width // LANES, 1), :] = jnp.sum(loss_acc[...], axis=0, keepdims=True)
            for d in range(1, n_tp):
                everyone(fin_buf, fin_send, fin_recv, d).start()

    def stage_d(c):
        rdma(c, K_OUT_R).wait_recv()
        rdma(c, K_PASS_R).start()
        rdma(c, K_FWD_L).start()
        rdma(c, K_OUT_L).wait_recv()
        rdma(c, K_PASS_L).start()
        rdma(c, K_FWD_R).start()

    def stage_e(c):
        rdma(c, K_PASS_R).wait_recv()
        rdma(c, K_PASS_L).wait_recv()
        rdma(c, K_FWD_O).start()

    def stage_f(c):
        for kind in (K_OUT_S, K_FWD_L, K_FWD_R, K_FWD_O):
            rdma(c, kind).wait_recv()
        dh_s[pl.ds(pl.multiple_of(c * CHUNK, CHUNK), CHUNK), :] = grad[c].astype(jnp.bfloat16)
        put_dh(c).start()

    stages = ((LAG_F, stage_f), (LAG_E, stage_e), (LAG_D, stage_d), (LAG_C, stage_c), (LAG_B, stage_b), (LAG_A, stage_a))

    @pl.loop(0, blocks - 1)
    def _(i):
        make_dz(0, i)

    last = SLOTS * (chunks - 1)

    @pl.loop(0, SLOTS * chunks + LAG_F - SLOTS + 1)
    def _(slot):
        for lag, stage in stages:
            since = slot - lag

            @pl.when((since >= 0) & (lax.rem(since + SLOTS * LAG_F, SLOTS) == 0) & (since < SLOTS * chunks))
            def _(since=since, stage=stage):
                stage(since // SLOTS)

        phase = lax.rem(slot, SLOTS)
        c = slot // SLOTS

        @pl.when((phase == 0) & (c < chunks - 1))
        def _():
            prepare(c + 1)

        @pl.when((c < chunks - 1))
        def _():
            first = jnp.where(phase == 0, 0, jnp.where(phase == 1, 1, (blocks + 1) // 2))
            count = jnp.where(phase == 0, 1, jnp.where(phase == 1, (blocks + 1) // 2 - 1, blocks - (blocks + 1) // 2))

            @pl.loop(0, count)
            def _(i):
                block = (c + 1) * blocks + first + i - 1
                make_dz(block // blocks, lax.rem(block, blocks))
                targets(first + i)

        @pl.when(slot == last)
        def _():
            make_dz(chunks - 1, blocks - 1)

        @pl.when((phase == 0) & (c < chunks))
        def _():
            make_dx(c)

    for d in range(1, n_tp):
        everyone(fin_buf, fin_send, fin_recv, d).wait_recv()
    fin = functools.reduce(jnp.add, [fin_buf[k] for k in range(n_tp)])
    lanes = width // LANES
    loss = jnp.sum(slz_acc[:, 0:1], axis=0, keepdims=True) - jnp.sum(fin[lanes:lanes + 1, :], axis=1, keepdims=True)
    fin_ref[...] = fin
    fin_ref[pl.ds(lanes, 1), :] = jnp.broadcast_to(loss, (1, LANES))

    for d in range(1, n_tp):
        everyone(stat_buf, stat_send, stat_recv, d).wait_send()
        everyone(fin_buf, fin_send, fin_recv, d).wait_send()

    @pl.loop(0, chunks)
    def _(c):
        for kind in range(KINDS):
            rdma(c, kind).wait_send()
        put_dh(c).wait()
        put_dz(c).wait()

    put_x.wait()


def solution(mesh):
    n_tp = mesh.shape['tp']

    def local_step(hidden, norm_gain, emb_block, teacher_ids, teacher_q):
        tokens, width = hidden.shape
        vocab = emb_block.shape[0]
        count = teacher_ids.shape[1]
        chunks = tokens // CHUNK
        half = CHUNK // 2
        bit = half // (n_tp // 2) // 2
        f32, bf16 = jnp.float32, jnp.bfloat16
        dma = pltpu.SemaphoreType.DMA
        hbm, vmem = pl.BlockSpec(memory_space=pl.ANY), pl.BlockSpec(memory_space=pltpu.VMEM)
        dh, x_in, grad_z, fin = pl.pallas_call(
            functools.partial(kernel, n_tp),
            out_shape=(jax.ShapeDtypeStruct((tokens, width), bf16), jax.ShapeDtypeStruct((tokens, width), bf16),
                       jax.ShapeDtypeStruct((tokens, vocab), bf16), jax.ShapeDtypeStruct((16, LANES), f32)),
            in_specs=[hbm, vmem, hbm, hbm, hbm],
            out_specs=(hbm, hbm, hbm, vmem),
            scratch_shapes=[
                pltpu.VMEM((tokens, width), bf16), pltpu.VMEM((vocab, width), bf16), pltpu.VMEM((tokens, count), jnp.int32), pltpu.VMEM((tokens, count), f32),
                pltpu.VMEM((tokens, width), bf16), pltpu.VMEM((vocab // BLOCK, tokens, BLOCK), f32), pltpu.VMEM((tokens, vocab), bf16), *[pltpu.VMEM((tokens, LANES), f32)] * 3,
                *[pltpu.VMEM((CHUNK, count), f32)] * 2, pltpu.VMEM((CHUNK * (vocab // LANES + 1), LANES), f32),
                pltpu.VMEM((chunks, CHUNK, width), f32), pltpu.VMEM((chunks, half, width), f32), pltpu.VMEM((chunks, 6, bit, width), f32),
                pltpu.VMEM((chunks, CHUNK, width), f32), pltpu.VMEM((tokens, width), bf16),
                pltpu.VMEM((8, width), f32), pltpu.VMEM((8, LANES), f32), pltpu.VMEM((8, LANES), f32),
                pltpu.VMEM((n_tp, 2 * tokens // LANES, LANES), f32), pltpu.VMEM((n_tp, 16, LANES), f32),
                dma((6,)), dma((vocab // BLOCK,)), dma((chunks,)), dma((chunks,)), dma(()),
                dma((n_tp - 1,)), dma((n_tp - 1,)), dma((n_tp - 1,)), dma((n_tp - 1,)), dma((chunks, KINDS)), dma((chunks, KINDS)),
            ],
            compiler_params=pltpu.CompilerParams(collective_id=0, has_side_effects=True, vmem_limit_bytes=60 * 2**20),
        )(hidden, norm_gain, emb_block, teacher_ids, teacher_q)
        grad_block = lax.dot_general(grad_z, x_in, (((0,), (0,)), ((), ())), preferred_element_type=f32)
        lanes = width // LANES
        return fin[lanes, :1], dh, fin[:lanes].reshape(-1), grad_block

    return jax.shard_map(local_step, mesh=mesh, in_specs=(P('dp', None), P(None), P('tp', None), P('dp', None), P('dp', None)), out_specs=(P('dp'), P('dp', None), P('dp'), P(('dp', 'tp'), None)), check_vma=False)
```
